32 devices in a mesh: dp: 2 (over z, core), tp: 16 (over x, y).
Axes of the slice: x: 4, y: 4, z: 1, core: 2. Of those that a mesh axis runs over, the one named last changes fastest.
The devices are a block of a 4x4x8 slice.
Arguments:
- x: bfloat16 [8192, 4096], P(('dp', 'tp')), parts along dimension 0
- dy: bfloat16 [8192, 4096], P(('dp', 'tp')), parts along dimension 0
- gate: bfloat16 [8192, 16384], P('dp', 'tp'), parts along dimension 0
- up: bfloat16 [8192, 16384], P('dp', 'tp'), parts along dimension 0
- w_gate: bfloat16 [4096, 16384], P(None, 'tp')
- w_up: bfloat16 [4096, 16384], P(None, 'tp')
- w_down: bfloat16 [16384, 4096], P('tp')
Outputs:
- output 1: bfloat16 [8192, 4096], P(('dp', 'tp')), parts along dimension 0
- output 2: bfloat16 [8192, 16384], P('dp', 'tp'), parts along dimension 0
- output 3: bfloat16 [8192, 16384], P('dp', 'tp'), parts along dimension 0
- output 4: bfloat16 [32768, 4096], P(('dp', 'tp')), parts along dimension 0
There are 2 independent parts. The reference program is written for one: setup_inputs(seed, part) draws one part's arguments, and reference() takes and returns one part's arrays. A program takes and returns all parts, laid end to end along the dimension named above; an argument that names none is the same for every part.
All inputs are finite; a program needn't handle non-finite values.
Results may differ from the reference program's by a relative error of at most 0.012.
Values are sent between devices in bfloat16 or wider.
A program may use at most 768 MiB of HBM per device.

```python
import jax
import jax.numpy as jnp

ROWS = 4096
D = 4096
FF = 16384


def act(gate, up):
    return jax.nn.silu(gate) * up


def setup_inputs(seed: int = 0, part: int = 0) -> dict:
    kx, ky, ka, kb, kg, ku, kd = jax.random.split(jax.random.key(seed), 7)
    kx, ky, ka, kb = (jax.random.fold_in(k, part) for k in (kx, ky, ka, kb))
    drawn = {
        "x": jax.random.normal(kx, (ROWS, D), jnp.float32),
        "dy": jax.random.normal(ky, (ROWS, D), jnp.float32),
        "gate": jax.random.normal(ka, (ROWS, FF), jnp.float32),
        "up": jax.random.normal(kb, (ROWS, FF), jnp.float32),
        "w_gate": jax.random.normal(kg, (D, FF), jnp.float32) * D**-0.5,
        "w_up": jax.random.normal(ku, (D, FF), jnp.float32) * D**-0.5,
        "w_down": jax.random.normal(kd, (FF, D), jnp.float32) * FF**-0.5,
    }
    return {k: v.astype(jnp.bfloat16) for k, v in drawn.items()}


def reference(x, dy, gate, up, w_gate, w_up, w_down):
    hidden, back = jax.vjp(act, gate.astype(jnp.float32), up.astype(jnp.float32))
    d_hidden = jnp.dot(dy, w_down.T, preferred_element_type=jnp.float32)
    d_gate, d_up = (g.astype(jnp.bfloat16) for g in back(d_hidden))
    dx = jnp.dot(d_gate, w_gate.T, preferred_element_type=jnp.float32) + jnp.dot(d_up, w_up.T, preferred_element_type=jnp.float32)
    dw_gate = jnp.dot(x.T, d_gate, preferred_element_type=jnp.float32)
    dw_up = jnp.dot(x.T, d_up, preferred_element_type=jnp.float32)
    dw_down = jnp.dot(hidden.astype(jnp.bfloat16).T, dy, preferred_element_type=jnp.float32)
    return tuple(g.astype(jnp.bfloat16) for g in (dx, dw_gate, dw_up, dw_down))
```

```python
import functools
import math

import jax
import jax.numpy as jnp
from jax import lax
from jax.experimental import pallas as pl
from jax.experimental.pallas import tpu as pltpu
from jax.sharding import PartitionSpec as P

MESH = pl.DeviceIdType.MESH
BF16 = jnp.bfloat16
F32 = jnp.float32
NT = (((1,), (1,)), ((), ()))
TN = (((0,), (0,)), ((), ()))
BOTH = (0, 1)
SUB = 2
PIECES = tuple(range(SUB))

X_AFTER = 9
X_START = (0, 6)
DURING_CHUNKS = ((0, 2, 2, 2), (0, 3, 4, 6), (0, 4, 6, 8), (0, 5, 8, 10), (0, 6, 10, 10), (1, 0, 12, 14))
DURING_DOWN = ((1, 1, 5, 6), (1, 2, 14, 15))
DURING_DX = ((1, 3, 6, 7), (1, 4, 15, 16), (1, 5, 25, 26))
SUMS_AT = (29, 18)


scope = jax.named_scope


def dot(a, b, dims):
    return lax.dot_general(a, b, dims, preferred_element_type=F32)


def kernel(
    side,
    x_in, dy_in, gate, up, wg, wu, wd,
    dx, og, ou, od, xg, dyg, cg, cu, cwg, cwu, cwd, dxp, dxr, rsl, crs,
    dgu, hid, wb, gu, out, xf, rin, rpx, rpr, rso,
    rsend, rrecv, dsend, drecv, csend, crecv, gsend, grecv,
    wsem, lsem, osem, orecv, xfs, xbs, drr, rss, rsr, rls, crr, csem,
):
    n = side
    ring_len = 2 * n
    rb, d_model = x_in.shape
    tok, ff = gate.shape
    hb = rb // 2
    fh = ff // 2
    kd = d_model // 2
    piece = hb // SUB
    blocks = tok // rb
    cq = d_model // 4

    t = lax.axis_index("tp")
    dp = lax.axis_index("dp")
    c = lax.rem(dp, 2)
    x = t // n
    y = lax.rem(t, n)
    s = lax.rem(x + y, n)
    team = s // 2
    odd = lax.rem(s, 2)
    swap = lax.rem(c + team, 2)
    stay = 1 - swap
    pdp = dp + 1 - 2 * c

    def on_stay(f):
        pl.when(stay == 1)(f)

    def on_swap(f):
        pl.when(swap == 1)(f)

    def wrap(v):
        return lax.rem(v + 2 * n, n)

    def wr(v):
        return lax.rem(v + 4 * ring_len, ring_len)

    def neighbours(x, y, odd):
        sg = 2 * odd - 1
        cx = wrap(x + sg) * n + y
        cy = x * n + wrap(y + sg)
        rx = wrap(x - sg) * n + y
        ry = x * n + wrap(y - sg)
        return cx, cy, rx * (1 - odd) + ry * odd, ry * (1 - odd) + rx * odd

    cx, cy, nxt, prv = neighbours(x, y, odd)
    links = (cx, cy)
    r = wr(2 * x - odd)

    def stay_f(q, team):
        q = wr(q)
        o = lax.rem(q, 2)
        bx = lax.rem((q + o) // 2, n)
        return bx * n + wrap(2 * team + o - bx)

    def swap_f(q, team):
        q = wr(q)
        o = lax.rem(q, 2)
        bx = lax.rem((q + 3 * o) // 2, n)
        return bx * n + wrap(2 * (1 - team) + (1 - o) - bx)

    def blk_f(q_stay, q_swap):
        return stay_f(q_stay, team) * stay + swap_f(q_swap, team) * swap

    def send_blk(dn, i):
        if dn == 0:
            return blk_f(r - i, r - i - (1 if i >= 1 else 0))
        return blk_f(r + i, r - 2 if i == 0 else r - 1 + i)

    def arr_blk(dn, k):
        if dn == 0:
            return blk_f(r - 1 - k, r - 1 if k == 0 else r - 2 - k)
        return blk_f(r + 1 + k, r - 1 if k == 0 else r + k)

    def chunk(j, team, r, t, cx, cy):
        k = jnp.maximum(j - 3, 0) // 2
        sw = jnp.where((j == 1) | (j == 2) | ((j >= 4) & (lax.rem(j, 2) == 0)), 1, 0)
        first = jnp.where(k == 0, 1, 0)
        st_a = jnp.where(j == 0, t, stay_f(r - 1 - k, team))
        st_b = jnp.where(j == 0, t, stay_f(r + 1 + k, team))
        entry = jnp.where(j == 1, cx, cy)
        sw_a = jnp.where(j < 3, entry, swap_f(r - 2 - k + first, team))
        sw_b = jnp.where(j < 3, entry, swap_f(r + k - first, team))
        return sw_a * sw + st_a * (1 - sw), sw_b * sw + st_b * (1 - sw), sw, k

    def al(v, m):
        return pl.multiple_of(v, m)

    bar = pltpu.get_barrier_semaphore()
    peers = ((dp, nxt), (dp, prv), (pdp, t), (pdp, cx), (pdp, cy))
    for p, f in peers:
        pl.semaphore_signal(bar, inc=1, device_id={"dp": p, "tp": f}, device_id_type=MESH)
    pl.semaphore_wait(bar, len(peers))

    ins = (dy_in, x_in)
    gath = (dyg, xg)
    nbr = (nxt, prv)

    def remote(src, dst, ssem, rsem, to_dp, to_tp):
        return pltpu.make_async_remote_copy(
            src, dst, ssem, rsem, device_id={"dp": to_dp, "tp": to_tp}, device_id_type=MESH
        )

    def rows_of(blk, dn, u):
        return pl.ds(al(blk * rb + (dn * hb + u * piece), piece), piece)

    def ring(a, dn, i, u, blk, own=False):
        dst = gath[a].at[rows_of(blk, dn, u)]
        src = ins[a].at[pl.ds(dn * hb + u * piece, piece)] if own else dst
        return remote(src, dst, rsend.at[a, dn, i, u], rrecv.at[a, dn, i, u], dp, nbr[dn])

    def d2d(a, dn, i, u, blk, own=False):
        dst = gath[a].at[rows_of(blk, dn, u)]
        src = ins[a].at[pl.ds(dn * hb + u * piece, piece)] if own else dst
        return remote(src, dst, dsend.at[a, dn, i, u], drecv.at[a, dn, i, u], pdp, t)

    def cross(l, j):
        cols = pl.ds(l * fh, fh)
        if j in (0, 1, 3, 4):
            a, h = (0, j) if j < 2 else (1, j - 3)
            src = ins[a].at[pl.ds(h * hb, hb)]
            dst = gath[a].at[pl.ds(al(t * rb + h * hb, hb), hb)]
        elif j == 2:
            src, dst = wd.at[cols], cwd.at[cols]
        elif j < 13:
            q = (j - 5) // 2
            w, cw = ((wg, cwg), (wu, cwu))[(j - 5) % 2]
            rows = pl.ds(q * cq, cq)
            src, dst = w.at[rows, cols], cw.at[rows, cols]
        else:
            src, dst = cwd.at[cols], od.at[cols]
        return remote(src, dst, csend.at[l, j], crecv.at[l, j], pdp, links[l])

    def cross_gu(l, j, h, a, f):
        rows = pl.ds(al(f * rb + h * hb, hb), hb)
        cols = pl.ds(l * fh, fh)
        src, dst = ((gate, cg), (up, cu))[a]
        return remote(src.at[rows, cols], dst.at[rows, cols], gsend.at[l, j, h, a], grecv.at[l, j, h, a], pdp, links[l])

    def their_chunk(l, j):
        f = links[l]
        fx, fy = f // n, lax.rem(f, n)
        f_odd = 1 - odd
        f_cx, f_cy, _, _ = neighbours(fx, fy, f_odd)
        f_a, f_b, _, _ = chunk(j, 1 - team, wr(2 * fx - f_odd), f, f_cx, f_cy)
        return f_a, f_b

    def cross_chunks(lo, hi):
        @pl.loop(lo, hi)
        def _(j):
            for l in BOTH:
                halves = their_chunk(l, j)
                for h in BOTH:
                    for a in BOTH:
                        cross_gu(l, j, h, a, halves[h]).start()

    @scope("ring_start")
    def ring_start(a):
        @on_stay
        def _():
            for u in PIECES:
                for dn in BOTH:
                    ring(a, dn, 0, u, t, own=True).start()
            for u in PIECES:
                for dn in BOTH:
                    d2d(a, dn, 7, u, t, own=True).start()

        @on_swap
        def _():
            for l in BOTH:
                for h in BOTH:
                    cross(l, 3 * a + h).wait_recv()
            for i in BOTH:
                for u in PIECES:
                    for dn in BOTH:
                        ring(a, dn, i, u, send_blk(dn, i)).start()
            for l in BOTH:
                for u in PIECES:
                    for dn in BOTH:
                        d2d(a, dn, 6 + l, u, links[l]).start()

    def ring_step(a, k):
        def body():
            for u in PIECES:
                for dn in BOTH:
                    b = arr_blk(dn, k)
                    ring(a, dn, k, u, b).wait_recv()

                    def forward():
                        ring(a, dn, k + 1, u, b).start()

                    if 1 <= k <= 4:
                        forward()
                    elif k < 6:
                        on_stay(forward)
                    d2d(a, dn, k, u, b).start()

        with scope(f"ring_{a}_{k}"):
            if k == 6:
                on_stay(body)
            else:
                body()

    def ring_steps(table, i):
        for a, k, on_stay_at, on_swap_at in table:

            @pl.when(i == on_stay_at * stay + on_swap_at * swap)
            def _():
                ring_step(a, k)
                if (a, k) == X_START:
                    ring_start(1)

    def bounce(a, h, kb, out_):
        vm = dgu.at[pl.ds((2 * a + kb) * rb + h * hb, hb), :]
        cols = pl.ds(kb * kd, kd)
        if out_:
            return pltpu.make_async_copy(vm, gath[a].at[pl.ds(al(t * rb + h * hb, hb), hb), cols], lsem.at[0, h, 2 * a + kb])
        return pltpu.make_async_copy(ins[a].at[pl.ds(h * hb, hb), cols], vm, lsem.at[0, h, 2 * a + kb])

    def wd_load(src, kb):
        return pltpu.make_async_copy(src.at[:, pl.ds(kb * kd, kd)], wb.at[1, pl.ds(kb * ff, ff), :], wsem.at[kb])

    early = blocks // 2

    @on_swap
    def _():
        for j in range(3):
            for l in BOTH:
                cross(l, j).start()
        cross_chunks(0, early)

    @on_stay
    def _():
        for a in BOTH:
            for h in BOTH:
                for kb in BOTH:
                    bounce(a, h, kb, False).start()
        for kb in BOTH:
            wd_load(wd, kb).start()

    ring_start(0)

    @on_stay
    def _():
        for out_ in (False, True):
            for a in BOTH:
                for h in BOTH:
                    for kb in BOTH:
                        bounce(a, h, kb, out_).wait()
                        if not out_:
                            bounce(a, h, kb, True).start()

    ring_step(0, 0)

    @on_swap
    def _():
        cross_chunks(early, X_AFTER)
        for j in (3, 4):
            for l in BOTH:
                cross(l, j).start()
        cross_chunks(X_AFTER, blocks)
        for j in range(5, 13):
            for l in BOTH:
                cross(l, j).start()

    ring_step(0, 1)

    @on_swap
    def _():
        for l in BOTH:
            cross(l, 2).wait_recv()
        for kb in BOTH:
            wd_load(cwd, kb).start()

    def chunk_load(j, slot, h, what, f):
        rows = pl.ds(al(f * rb + h * hb, hb), hb)
        sem = lsem.at[slot, h, what]
        if what < 2:
            dst = wb.at[0, pl.ds(al(slot * 2 * rb + what * rb + h * hb, hb), hb), :]
            return pltpu.make_async_copy(dyg.at[rows, pl.ds(what * kd, kd)], dst, sem)
        dst = gu.at[slot, what % 2, pl.ds(h * hb, hb), :]
        src = ((gate, up), (cg, cu))[what // 4][what % 2]
        return pltpu.make_async_copy(src.at[rows, :], dst, lsem.at[slot, h, 2 + what % 2])

    @scope("chunk_start")
    def chunk_start(j):
        slot = lax.rem(j, 2)
        f_a, f_b, sw, k = chunk(j, team, r, t, cx, cy)
        halves = (f_a, f_b)

        @pl.when(sw != swap)
        def _():
            idx = jnp.where(j == 0, 7, jnp.where(j < 3, 5 + j, k))
            for dn in BOTH:
                for u in PIECES:
                    d2d(0, dn, idx, u, halves[dn]).wait_recv()

        for h in BOTH:
            for kb in BOTH:
                chunk_load(j, slot, h, kb, halves[h]).start()

        @on_stay
        def _():
            for h in BOTH:
                for a in BOTH:
                    chunk_load(j, slot, h, 2 + a, halves[h]).start()

        @on_swap
        def _():
            for l in BOTH:
                for h in BOTH:
                    for a in BOTH:
                        cross_gu(l, j, h, a, halves[h]).wait_recv()
            for h in BOTH:
                for a in BOTH:
                    chunk_load(j, slot, h, 4 + a, halves[h]).start()

    @scope("chunk")
    def chunk_compute(j):
        slot = lax.rem(j, 2)
        f_a, f_b, _, _ = chunk(j, team, r, t, cx, cy)
        halves = (f_a, f_b)
        for h in BOTH:
            for what in range(4):
                chunk_load(j, slot, h, what, halves[h]).wait()
        for nt in BOTH:
            cols = pl.ds(nt * fh, fh)
            lhs = al(slot * 2 * rb, 2 * rb)
            dh = dot(wb[0, pl.ds(lhs, rb), :], wb[1, pl.ds(nt * fh, fh), :], NT)
            dh += dot(wb[0, pl.ds(lhs + rb, rb), :], wb[1, pl.ds(ff + nt * fh, fh), :], NT)
            g = gu[slot, 0, :, cols].astype(F32)
            u = gu[slot, 1, :, cols].astype(F32)
            sig = jax.nn.sigmoid(g)
            act = g * sig
            d_up = (dh * act).astype(BF16)
            d_gate = ((dh * u) * (sig * (1.0 + g * (1.0 - sig)))).astype(BF16)
            hidden = (act * u).astype(BF16)
            for h in BOTH:
                rows = pl.ds(al(halves[h] * rb + h * hb, hb), hb)
                part = slice(h * hb, (h + 1) * hb)
                dgu[rows, nt * fh : (nt + 1) * fh] = d_gate[part]
                dgu[rows, ff + nt * fh : ff + (nt + 1) * fh] = d_up[part]
                hid[rows, nt * fh : (nt + 1) * fh] = hidden[part]

    chunk_start(0)

    @on_stay
    def _():
        chunk_start(1)

    for kb in BOTH:
        wd_load(wd, kb).wait()

    @pl.loop(0, blocks)
    def _(j):
        chunk_compute(j)
        ring_steps(DURING_CHUNKS, j)

        @pl.when(j + 1 + stay < blocks)
        def _():
            chunk_start(j + 1 + stay)

    half = tok // 2

    def dy_cols(q, slot, th):
        return pltpu.make_async_copy(
            dyg.at[pl.ds(th * half, half), pl.ds(al(q * cq, cq), cq)],
            wb.at[slot, :, pl.ds(th * cq, cq)],
            wsem.at[2 * slot + th],
        )

    def dd_out(i, to):
        rows = pl.ds(al(lax.rem(i, 4) * rb, rb), rb)
        cols = pl.ds(al((i // 4) * cq, cq), cq)
        o = lax.rem(i, 4)
        return pltpu.make_async_copy(out.at[o, 0], to.at[rows, cols], osem.at[o, 0, 0])

    for q in BOTH:
        for th in BOTH:
            dy_cols(q, q, th).start()

    @scope("dw_down")
    def down_tile(i):
        q = i // 4
        ft = lax.rem(i, 4)
        slot = lax.rem(q, 2)

        @pl.when(ft == 0)
        def _():
            for th in BOTH:
                dy_cols(q, slot, th).wait()

            @pl.when((q == 1) | (q == 2))
            def _():
                for th in BOTH:
                    dy_cols(q + 1, 1 - slot, th).start()

        @pl.when(i >= 4)
        def _():
            dd_out(i - 4, od).wait()

        cols = pl.ds(al(ft * rb, rb), rb)
        o = dot(hid[0:half, cols], wb[slot, :, 0:cq], TN)
        o += dot(hid[half:tok, cols], wb[slot, :, cq : 2 * cq], TN)
        out[ft, 0] = o.astype(BF16)

        @on_stay
        def _():
            dd_out(i, od).start()

        @on_swap
        def _():
            dd_out(i, cwd).start()

    def w_load(q, a, src):
        rows = pl.ds(al(q * cq, cq), cq)
        slot = lax.rem(q, 2)
        return pltpu.make_async_copy(
            src.at[rows, :], wb.at[0, pl.ds(al(slot * cq, cq), cq), pl.ds(a * ff, ff)], wsem.at[4 + 2 * slot + a]
        )

    def cross_w(q, l, a):
        rows = pl.ds(al(q * cq, cq), cq)
        cols = pl.ds(l * fh, fh)
        src, dst = ((wg, cwg), (wu, cwu))[a]
        j = 5 + 2 * q + a
        return remote(src.at[rows, cols], dst.at[rows, cols], csend.at[l, j], crecv.at[l, j], pdp, links[l])

    @scope("w_start")
    def w_start(q):
        @on_stay
        def _():
            for a in BOTH:
                w_load(q, a, (wg, wu)[a]).start()

        @on_swap
        def _():
            for a in BOTH:
                for l in BOTH:
                    cross_w(q, l, a).wait_recv()
                w_load(q, a, (cwg, cwu)[a]).start()

    @pl.loop(0, 16)
    def _(i):
        @pl.when(i == 12)
        def _():
            w_start(0)

        down_tile(i)
        ring_steps(DURING_DOWN, i)

    for i in range(12, 16):
        dd_out(i, od).wait()

    @on_swap
    def _():
        for l in BOTH:
            cross(l, 13).start()

    def own_f(i):
        return blk_f(i, i)

    def other_f(i):
        return stay_f(i, team) * swap + swap_f(i, team) * stay

    def xf_out(step):
        q, i, o = step // ring_len, lax.rem(step, ring_len), lax.rem(step, 2)
        rows = pl.ds(al(own_f(i) * rb, rb), rb)
        return pltpu.make_async_copy(xf.at[o], dxp.at[rows, pl.ds(al(q * cq, cq), cq)], xfs.at[o])

    def xb_out(q, i, o):
        rows = pl.ds(al(other_f(i) * rb, rb), rb)
        return remote(out.at[o, 0], dxr.at[rows, pl.ds(al(q * cq, cq), cq)], xbs.at[o], drr.at[q, i], pdp, t)

    def xb_send(step):
        return xb_out(step // ring_len, lax.rem(step, ring_len), lax.rem(step, 2))

    def rs_nbr(dn):
        return prv * (1 - dn) + nxt * dn

    def rs_send(dn, k, u, slot):
        return remote(rso.at[slot], rsl.at[dn, k, u], rss.at[slot], rsr.at[dn, k, u], dp, rs_nbr(dn))

    def slot_free(slot):
        pltpu.make_async_copy(rso.at[slot], rso.at[slot], rss.at[slot]).wait()

    def rs_part(which, slot, blk, dn, u):
        rows = pl.ds(al(blk * rb + dn * hb, hb), hb)
        cols = pl.ds(al(u * kd, kd), kd)
        src, dst = ((dxp, rpx), (dxr, rpr))[which]
        return pltpu.make_async_copy(src.at[rows, cols], dst.at[slot], rls.at[slot, which])

    def rs_sum(slot, to, received):
        @pl.loop(0, hb // 16)
        def _(i):
            rows = pl.ds(al(i * 16, 16), 16)
            v = rpx[slot, rows, :] + rpr[slot, rows, :].astype(F32)
            if received:
                v += rin[slot, rows, :].astype(F32)
            rso[to, rows, :] = v.astype(BF16)

    @scope("sum_start")
    def rs_start(u):
        for q in (2 * u, 2 * u + 1):
            for i in range(ring_len):
                own = pl.ds(al(own_f(i) * rb, rb), rb)
                remote(out.at[0, 0], dxr.at[own, pl.ds(q * cq, cq)], xbs.at[0], drr.at[q, i], pdp, t).wait_recv()

        def first(blks, k, base):
            for dn in BOTH:
                for which in BOTH:
                    rs_part(which, dn, blks[dn], dn, u).start()
            for dn in BOTH:
                for which in BOTH:
                    rs_part(which, dn, blks[dn], dn, u).wait()
                slot = base + 2 * u + dn
                rs_sum(dn, slot, False)
                rs_send(dn, k, u, slot).start()

        first((blk_f(r + 1, r + 1), blk_f(r - 1, r + 5)), 0, 0)

        @on_swap
        def _():
            first((swap_f(r - 1, team), swap_f(r - 1, team)), 5, 4)

    def rs_place(tt):
        k = tt // 4
        u = lax.rem(tt, 4) // 2
        dn = lax.rem(tt, 2)
        late = jnp.where(k == 5, 1, 0)
        q_stay = (r - 6 + k) * (1 - dn) + (r + 6 - k) * dn
        q_swap = (r - 6 + k + late) * (1 - dn) + (r + 4 - k - late) * dn
        return k, u, dn, blk_f(q_stay, q_swap)

    def rs_in(dn, k, u, slot):
        return pltpu.make_async_copy(rsl.at[dn, k, u], rin.at[slot], rls.at[slot, 2])

    @scope("sum_take")
    def rs_take(tt, slot):
        k, u, dn, blk = rs_place(tt)

        @pl.when((stay == 1) | (k < 6))
        def _():
            rs_part(0, slot, blk, dn, u).start()
            rs_part(1, slot, blk, dn, u).start()
            rs_send(dn, k, u, 0).wait_recv()
            rs_in(dn, k, u, slot).start()

    def dx_out(dn, u, slot):
        cols = pl.ds(al(u * kd, kd), kd)
        return pltpu.make_async_copy(rso.at[slot], dx.at[pl.ds(al(dn * hb, hb), hb), cols], rss.at[slot])

    def rs_back(l, dn, u, slot):
        return remote(rso.at[slot], crs.at[l, dn, u], rss.at[slot], crr.at[l, dn, u], pdp, cx * (1 - l) + cy * l)

    @scope("sum_give")
    def rs_give(tt, slot):
        k, u, dn, blk = rs_place(tt)
        to = lax.rem(tt, 8)

        @pl.when((stay == 1) | (k < 6))
        def _():
            rs_part(0, slot, blk, dn, u).wait()
            rs_part(1, slot, blk, dn, u).wait()
            rs_in(dn, k, u, slot).wait()

            @pl.when((k != 1) | (swap == 1))
            def _():
                slot_free(to)

            rs_sum(slot, to, True)

            @pl.when(k < 4 + 2 * stay)
            def _():
                rs_send(dn, k + 1, u, to).start()

            @pl.when(k == 6)
            def _():
                dx_out(dn, u, to).start()

            @pl.when((swap == 1) & (k >= 4))
            def _():
                is_r = (k - 4) * (1 - dn) + (5 - k) * dn
                rs_back(lax.rem(is_r + odd, 2), dn, u, to).start()

    @pl.loop(0, 4 * ring_len)
    @scope("dx")
    def _(step):
        q = step // ring_len
        i = lax.rem(step, ring_len)
        o = lax.rem(step, 2)

        @pl.when(step == SUMS_AT[0] * stay + SUMS_AT[1] * swap)
        def _():
            rs_start(0)

        @pl.when(i == 0)
        def _():
            for a in BOTH:
                w_load(q, a, wg).wait()

        @pl.when((i == 5) & (q < 3))
        def _():
            w_start(q + 1)

        @pl.when(step >= 2)
        def _():
            xf_out(step - 2).wait()
            xb_send(step - 2).wait_send()

        w = pl.ds(al(lax.rem(q, 2) * cq, cq), cq)
        rows = pl.ds(al(own_f(i) * rb, rb), rb)
        xf[o] = dot(dgu[rows, :], wb[0, w, :], NT)
        xf_out(step).start()
        rows = pl.ds(al(other_f(i) * rb, rb), rb)
        out[o, 0] = dot(dgu[rows, :], wb[0, w, :], NT).astype(BF16)
        xb_send(step).start()
        ring_steps(DURING_DX, step)

    for step in (4 * ring_len - 2, 4 * ring_len - 1):
        xf_out(step).wait()
        xb_send(step).wait_send()

    ring_step(1, 6)
    rs_start(1)
    for dn in BOTH:
        for i in range(8):
            for u in PIECES:
                d2d(1, dn, i, u, t).wait_recv()

    def x_cols(i):
        slot = lax.rem(i, 4)
        return pltpu.make_async_copy(
            xg.at[:, pl.ds(al(i * rb, rb), rb)], hid.at[:, pl.ds(al(slot * rb, rb), rb)], wsem.at[slot]
        )

    def dw_local(i, a):
        o = lax.rem(i, 4)
        return pltpu.make_async_copy(out.at[o, a], (og, ou)[a].at[pl.ds(al(i * rb, rb), rb), :], osem.at[o, a, 0])

    def dw_remote(i, a, l):
        o = lax.rem(i, 4)
        rows = pl.ds(al(i * rb, rb), rb)
        cols = pl.ds(l * fh, fh)
        return remote(out.at[o, a, :, cols], (og, ou)[a].at[rows, cols], osem.at[o, a, l], orecv.at[l, a, i], pdp, links[l])

    def dw_start(i, a):
        @on_stay
        def _():
            dw_local(i, a).start()

        @on_swap
        def _():
            for l in BOTH:
                dw_remote(i, a, l).start()

    @scope("dw_wait")
    def dw_wait(i, a):
        @on_stay
        def _():
            dw_local(i, a).wait()

        @on_swap
        def _():
            for l in BOTH:
                dw_remote(i, a, l).wait_send()

    for i in range(3):
        x_cols(i).start()

    @pl.loop(0, blocks)
    @scope("dw")
    def _(i):
        o = lax.rem(i, 4)

        @pl.when(i + 3 < blocks)
        def _():
            x_cols(i + 3).start()

        x_cols(i).wait()
        rs_take(i, 0)
        for a in BOTH:

            @pl.when(i >= 4)
            def _():
                dw_wait(i - 4, a)

            lhs = hid[:, pl.ds(al(o * rb, rb), rb)]
            out[o, a] = dot(lhs, dgu[:, a * ff : (a + 1) * ff], TN).astype(BF16)
            dw_start(i, a)
            if a == 0:
                rs_give(i, 0)

    @pl.loop(blocks, 28)
    def _(tt):
        rs_take(tt, 0)
        rs_give(tt, 0)

    @on_swap
    def _():
        for u in BOTH:
            for dn in BOTH:
                slot = 2 * u + dn
                for l in BOTH:
                    rs_back(l, dn, u, 0).wait_recv()
                pltpu.make_async_copy(crs.at[0, dn, u], rin.at[0], csem.at[0]).start()
                pltpu.make_async_copy(crs.at[1, dn, u], rin.at[1], csem.at[1]).start()
                pltpu.make_async_copy(crs.at[0, dn, u], rin.at[0], csem.at[0]).wait()
                pltpu.make_async_copy(crs.at[1, dn, u], rin.at[1], csem.at[1]).wait()
                slot_free(slot)

                @pl.loop(0, hb // 16)
                def _(i):
                    rows = pl.ds(al(i * 16, 16), 16)
                    rso[slot, rows, :] = (rin[0, rows, :].astype(F32) + rin[1, rows, :].astype(F32)).astype(BF16)

                dx_out(dn, u, slot).start()

    for i in range(blocks - 4, blocks):
        for a in BOTH:
            dw_wait(i, a)
    for slot in range(8):
        slot_free(slot)
    for a in BOTH:
        for dn in BOTH:
            for u in PIECES:
                for k in range(6):
                    ring(a, dn, k, u, t).wait_send()
                for k in range(8):
                    d2d(a, dn, k, u, t).wait_send()

    @on_stay
    def _():
        for a in BOTH:
            for dn in BOTH:
                for u in PIECES:
                    ring(a, dn, 6, u, t).wait_send()

    @on_swap
    def _():
        for l in BOTH:
            for j in range(14):
                cross(l, j).wait_send()
            cross(l, 13).wait_recv()

            @pl.loop(0, blocks)
            def _(j):
                for h in BOTH:
                    for a in BOTH:
                        cross_gu(l, j, h, a, t).wait_send()
                for a in BOTH:
                    dw_remote(j, a, l).wait_recv()


def copy_out(*refs):
    count = len(refs) // 4
    srcs, dsts, bufs, sems = (refs[i * count : (i + 1) * count] for i in range(4))
    moves = []
    for src, dst, buf, sem in zip(srcs, dsts, bufs, sems):
        pieces = sem.shape[1]
        rows = src.shape[0] // pieces
        for i in range(pieces):
            at = pl.ds(i * rows, rows)
            moves.append(
                (
                    pltpu.make_async_copy(src.at[at], buf.at[at], sem.at[0, i]),
                    pltpu.make_async_copy(buf.at[at], dst.at[at], sem.at[1, i]),
                )
            )
    for load, _ in moves:
        load.start()
    for load, store in moves:
        load.wait()
        store.start()
    for _, store in moves:
        store.wait()


def solution(mesh):
    side = math.isqrt(mesh.shape["tp"])

    def local(x, dy, gate, up, wg, wu, wd):
        rb, d = x.shape
        tok, ff = gate.shape
        hb, kd, blocks = rb // 2, d // 2, tok // rb

        def hbm(*shape, dtype=BF16):
            return jax.ShapeDtypeStruct(shape, dtype)

        outs = [
            hbm(rb, d), hbm(d, ff), hbm(d, ff), hbm(ff, d),
            hbm(tok, d), hbm(tok, d),
            hbm(tok, ff), hbm(tok, ff), hbm(d, ff), hbm(d, ff), hbm(ff, d),
            hbm(tok, d, dtype=F32), hbm(tok, d),
            hbm(2, 7, 2, hb, kd), hbm(2, 2, 2, hb, kd),
        ]
        sem = pltpu.SemaphoreType.DMA
        scratch = [
            pltpu.VMEM((tok, 2 * ff), BF16),
            pltpu.VMEM((tok, ff), BF16),
            pltpu.VMEM((2, tok // 2, kd), BF16),
            pltpu.VMEM((2, 2, rb, ff), BF16),
            pltpu.VMEM((4, 2, rb, ff), BF16),
            pltpu.VMEM((2, rb, d // 4), F32),
            pltpu.VMEM((2, hb, kd), BF16),
            pltpu.VMEM((2, hb, kd), F32),
            pltpu.VMEM((2, hb, kd), BF16),
            pltpu.VMEM((8, hb, kd), BF16),
            sem((2, 2, 7, SUB)), sem((2, 2, 7, SUB)), sem((2, 2, 8, SUB)), sem((2, 2, 8, SUB)),
            sem((2, 14)), sem((2, 14)), sem((2, blocks, 2, 2)), sem((2, blocks, 2, 2)),
            sem((8,)), sem((2, 2, 4)), sem((4, 2, 2)), sem((2, 2, blocks)),
            sem((2,)), sem((2,)), sem((4, 2 * side)), sem((8,)), sem((2, 7, 2)), sem((2, 3)), sem((2, 2, 2)), sem((2,)),
        ]
        res = pl.pallas_call(
            functools.partial(kernel, side),
            out_shape=outs,
            in_specs=[pl.BlockSpec(memory_space=pl.ANY)] * 7,
            out_specs=[pl.BlockSpec(memory_space=pl.ANY)] * len(outs),
            scratch_shapes=scratch,
            compiler_params=pltpu.CompilerParams(
                collective_id=0, has_side_effects=True, vmem_limit_bytes=64 * 2**20 - 2**16
            ),
            name="gated_mlp_backward",
        )(x, dy, gate, up, wg, wu, wd)
        res = res[:4]
        anywhere = [pl.BlockSpec(memory_space=pl.ANY)] * len(res)
        return pl.pallas_call(
            copy_out,
            out_shape=[hbm(*v.shape) for v in res],
            in_specs=anywhere,
            out_specs=anywhere,
            scratch_shapes=[pltpu.VMEM(v.shape, BF16) for v in res]
            + [sem((2, max(1, v.size // (4 * rb * ff)))) for v in res],
            compiler_params=pltpu.CompilerParams(vmem_limit_bytes=48 * 2**20),
            name="copy_out",
        )(*res)

    rows, cols = P(("dp", "tp"), None), P("dp", "tp")
    return jax.shard_map(
        local,
        mesh=mesh,
        in_specs=(rows, rows, cols, cols, P(None, "tp"), P(None, "tp"), P("tp", None)),
        out_specs=(rows, cols, cols, rows),
        check_vma=False,
    )
```

```python
import functools
import math

import jax
import jax.numpy as jnp
from jax import lax
from jax.experimental import pallas as pl
from jax.experimental.pallas import tpu as pltpu
from jax.sharding import PartitionSpec as P

MESH = pl.DeviceIdType.MESH
BF16 = jnp.bfloat16
F32 = jnp.float32
NT = (((1,), (1,)), ((), ()))
TN = (((0,), (0,)), ((), ()))
BOTH = (0, 1)
SUB = 2
PIECES = tuple(range(SUB))

X_AFTER = 9
START = -1
SUMS = -2
NEVER = -1
DURING_CHUNKS = (
    (0, 2, 2, 2), (0, 3, 4, 6), (0, 4, 6, 8), (0, 5, 8, 10), (0, 6, 10, NEVER),
    (1, START, 10, 10), (1, 0, 12, 14),
)
DURING_DOWN = ((1, 1, 3, 5),)
DURING_DX = ((1, 2, 5, 6), (1, 3, 14, 14), (1, 4, 23, 22), (1, 5, 31, 30), (1, SUMS, 31, 23))


scope = jax.named_scope


def dot(a, b, dims):
    return lax.dot_general(a, b, dims, preferred_element_type=F32)


def kernel(
    side,
    x_in, dy_in, gate, up, wg, wu, wd,
    dx, og, ou, od, xg, dyg, cg, cu, cwg, cwu, cwd, dxp, dxr, rsl, crs,
    dgu, hid, wb, gu, out, xf, rin, rpx, rpr, rso,
    rsend, rrecv, dsend, drecv, csend, crecv, grecv,
    wsem, lsem, osem, orecv, xfs, xbs, drr, rss, rsr, rls, crr, csem, dsem,
):
    n = side
    ring_len = 2 * n
    rb, d_model = x_in.shape
    tok, ff = gate.shape
    hb = rb // 2
    fh = ff // 2
    kd = d_model // 2
    piece = hb // SUB
    blocks = tok // rb
    cq = d_model // 4

    t = lax.axis_index("tp")
    dp = lax.axis_index("dp")
    c = lax.rem(dp, 2)
    x = t // n
    y = lax.rem(t, n)
    s = lax.rem(x + y, n)
    team = s // 2
    odd = lax.rem(s, 2)
    swap = lax.rem(c + team, 2)
    stay = 1 - swap
    pdp = dp + 1 - 2 * c

    def on_stay(f):
        pl.when(stay == 1)(f)

    def on_swap(f):
        pl.when(swap == 1)(f)

    def wrap(v):
        return lax.rem(v + 2 * n, n)

    def wr(v):
        return lax.rem(v + 4 * ring_len, ring_len)

    def neighbours(x, y, odd):
        sg = 2 * odd - 1
        cx = wrap(x + sg) * n + y
        cy = x * n + wrap(y + sg)
        rx = wrap(x - sg) * n + y
        ry = x * n + wrap(y - sg)
        return cx, cy, rx * (1 - odd) + ry * odd, ry * (1 - odd) + rx * odd

    cx, cy, nxt, prv = neighbours(x, y, odd)
    links = (cx, cy)
    r = wr(2 * x - odd)

    def stay_f(q, team):
        q = wr(q)
        o = lax.rem(q, 2)
        bx = lax.rem((q + o) // 2, n)
        return bx * n + wrap(2 * team + o - bx)

    def swap_f(q, team):
        q = wr(q)
        o = lax.rem(q, 2)
        bx = lax.rem((q + 3 * o) // 2, n)
        return bx * n + wrap(2 * (1 - team) + (1 - o) - bx)

    def blk_f(q_stay, q_swap):
        return stay_f(q_stay, team) * stay + swap_f(q_swap, team) * swap

    def send_blk(dn, i):
        if dn == 0:
            return blk_f(r - i, r - i - (1 if i >= 1 else 0))
        return blk_f(r + i, r - 2 if i == 0 else r - 1 + i)

    def arr_blk(dn, k):
        if dn == 0:
            return blk_f(r - 1 - k, r - 1 if k == 0 else r - 2 - k)
        return blk_f(r + 1 + k, r - 1 if k == 0 else r + k)

    def chunk(j, team, r, t, cx, cy):
        k = jnp.maximum(j - 3, 0) // 2
        sw = jnp.where((j == 1) | (j == 2) | ((j >= 4) & (lax.rem(j, 2) == 0)), 1, 0)
        first = jnp.where(k == 0, 1, 0)
        st_a = jnp.where(j == 0, t, stay_f(r - 1 - k, team))
        st_b = jnp.where(j == 0, t, stay_f(r + 1 + k, team))
        entry = jnp.where(j == 1, cx, cy)
        sw_a = jnp.where(j < 3, entry, swap_f(r - 2 - k + first, team))
        sw_b = jnp.where(j < 3, entry, swap_f(r + k - first, team))
        return sw_a * sw + st_a * (1 - sw), sw_b * sw + st_b * (1 - sw), sw, k

    def al(v, m):
        return pl.multiple_of(v, m)

    bar = pltpu.get_barrier_semaphore()
    peers = ((dp, nxt), (dp, prv), (pdp, t), (pdp, cx), (pdp, cy))
    for p, f in peers:
        pl.semaphore_signal(bar, inc=1, device_id={"dp": p, "tp": f}, device_id_type=MESH)
    pl.semaphore_wait(bar, len(peers))

    ins = (dy_in, x_in)
    gath = (dyg, xg)
    nbr = (nxt, prv)

    def remote(src, dst, ssem, rsem, to_dp, to_tp):
        return pltpu.make_async_remote_copy(
            src, dst, ssem, rsem, device_id={"dp": to_dp, "tp": to_tp}, device_id_type=MESH
        )

    def rows_of(blk, dn, u):
        return pl.ds(al(blk * rb + (dn * hb + u * piece), piece), piece)

    def ring(a, dn, i, u, blk, own=False):
        dst = gath[a].at[rows_of(blk, dn, u)]
        src = ins[a].at[pl.ds(dn * hb + u * piece, piece)] if own else dst
        return remote(src, dst, rsend.at[a], rrecv.at[a, dn, i, u], dp, nbr[dn])

    def d2d(a, dn, i, u, blk, own=False):
        dst = gath[a].at[rows_of(blk, dn, u)]
        src = ins[a].at[pl.ds(dn * hb + u * piece, piece)] if own else dst
        return remote(src, dst, dsend.at[a], drecv.at[a, i], pdp, t)

    def d2d_wait(a, i):
        pltpu.make_async_copy(dyg.at[pl.ds(0, rb)], gath[a].at[pl.ds(0, rb)], drecv.at[a, i]).wait()

    def cross(l, j):
        cols = pl.ds(l * fh, fh)
        if j < 2:
            src, dst = ins[j], gath[j].at[pl.ds(al(t * rb, rb), rb)]
        else:
            src, dst = wd.at[cols], cwd.at[cols]
        return remote(src, dst, csend.at[l], crecv.at[l, j], pdp, links[l])

    def down_send(l, q):
        at = (pl.ds(l * fh, fh), pl.ds(q * cq, cq))
        return remote(cwd.at[at], od.at[at], csend.at[l], orecv.at[l], pdp, links[l])

    def cross_w(q, l, a):
        rows = pl.ds(al(q * cq, cq), cq)
        cols = pl.ds(l * fh, fh)
        src, dst = ((wg, cwg), (wu, cwu))[a]
        return remote(src.at[rows, cols], dst.at[rows, cols], csend.at[l], crecv.at[l, 3 + 2 * q + a], pdp, links[l])

    def cross_gu(l, j, h, a, f):
        rows = pl.ds(al(f * rb + h * hb, hb), hb)
        cols = pl.ds(l * fh, fh)
        src, dst = ((gate, cg), (up, cu))[a]
        return remote(src.at[rows, cols], dst.at[rows, cols], csend.at[l], grecv.at[j], pdp, links[l])

    def their_chunk(l, j):
        f = links[l]
        fx, fy = f // n, lax.rem(f, n)
        f_odd = 1 - odd
        f_cx, f_cy, _, _ = neighbours(fx, fy, f_odd)
        f_a, f_b, _, _ = chunk(j, 1 - team, wr(2 * fx - f_odd), f, f_cx, f_cy)
        return f_a, f_b

    def cross_chunks(lo, hi):
        @pl.loop(lo, hi)
        def _(j):
            for l in BOTH:
                halves = their_chunk(l, j)
                for h in BOTH:
                    for a in BOTH:
                        cross_gu(l, j, h, a, halves[h]).start()

    @scope("ring_start")
    def ring_start(a):
        @on_stay
        def _():
            for u in PIECES:
                for dn in BOTH:
                    ring(a, dn, 0, u, t, own=True).start()
            for u in PIECES:
                for dn in BOTH:
                    d2d(a, dn, 7, u, t, own=True).start()

        @on_swap
        def _():
            for l in BOTH:
                cross(l, a).wait_recv()
            for i in BOTH:
                for u in PIECES:
                    for dn in BOTH:
                        ring(a, dn, i, u, send_blk(dn, i)).start()
            for l in BOTH:
                for u in PIECES:
                    for dn in BOTH:
                        d2d(a, dn, 6 + l, u, links[l]).start()

    def ring_step(a, k):
        def body():
            for u in PIECES:
                for dn in BOTH:
                    b = arr_blk(dn, k)
                    ring(a, dn, k, u, b).wait_recv()

                    def forward():
                        ring(a, dn, k + 1, u, b).start()

                    if 1 <= k <= 4:
                        forward()
                    elif k < 6:
                        on_stay(forward)
                    d2d(a, dn, k, u, b).start()

        with scope(f"ring_{a}_{k}"):
            if k == 6:
                on_stay(body)
            else:
                body()

    def ring_steps(table, i):
        for a, k, on_stay_at, on_swap_at in table:

            @pl.when(i == on_stay_at * stay + on_swap_at * swap)
            def _():
                if k == SUMS:
                    rs_start(0)
                elif k == START:
                    ring_start(a)
                else:
                    ring_step(a, k)

    def bounce(a, h, kb, out_):
        vm = dgu.at[pl.ds((2 * a + kb) * rb + h * hb, hb), :]
        cols = pl.ds(kb * kd, kd)
        if out_:
            return pltpu.make_async_copy(vm, gath[a].at[pl.ds(al(t * rb + h * hb, hb), hb), cols], lsem.at[0, h, 2 * a + kb])
        return pltpu.make_async_copy(ins[a].at[pl.ds(h * hb, hb), cols], vm, lsem.at[0, h, 2 * a + kb])

    def wd_load(src, kb):
        return pltpu.make_async_copy(src.at[:, pl.ds(kb * kd, kd)], wb.at[1, pl.ds(kb * ff, ff), :], wsem.at[kb])

    early = blocks // 2

    @on_swap
    def _():
        for j in (0, 2):
            for l in BOTH:
                cross(l, j).start()
        cross_chunks(0, early)

    @on_stay
    def _():
        for a in BOTH:
            for h in BOTH:
                for kb in BOTH:
                    bounce(a, h, kb, False).start()
        for kb in BOTH:
            wd_load(wd, kb).start()

    ring_start(0)

    @on_stay
    def _():
        for out_ in (False, True):
            for a in BOTH:
                for h in BOTH:
                    for kb in BOTH:
                        bounce(a, h, kb, out_).wait()
                        if not out_:
                            bounce(a, h, kb, True).start()

    ring_step(0, 0)

    @on_swap
    def _():
        cross_chunks(early, X_AFTER)
        for l in BOTH:
            cross(l, 1).start()
        cross_chunks(X_AFTER, blocks)

        @pl.loop(0, 4)
        def _(q):
            for a in BOTH:
                for l in BOTH:
                    cross_w(q, l, a).start()

    ring_step(0, 1)

    @on_swap
    def _():
        for l in BOTH:
            cross(l, 2).wait_recv()
        for kb in BOTH:
            wd_load(cwd, kb).start()

    def chunk_load(j, slot, h, what, f):
        rows = pl.ds(al(f * rb + h * hb, hb), hb)
        sem = lsem.at[slot, h, what]
        if what < 2:
            dst = wb.at[0, pl.ds(al(slot * 2 * rb + what * rb + h * hb, hb), hb), :]
            return pltpu.make_async_copy(dyg.at[rows, pl.ds(what * kd, kd)], dst, sem)
        dst = gu.at[slot, what % 2, pl.ds(h * hb, hb), :]
        src = ((gate, up), (cg, cu))[what // 4][what % 2]
        return pltpu.make_async_copy(src.at[rows, :], dst, lsem.at[slot, h, 2 + what % 2])

    @scope("chunk_start")
    def chunk_start(j):
        slot = lax.rem(j, 2)
        f_a, f_b, sw, k = chunk(j, team, r, t, cx, cy)
        halves = (f_a, f_b)

        @pl.when(sw != swap)
        def _():
            idx = jnp.where(j == 0, 7, jnp.where(j < 3, 5 + j, k))
            d2d_wait(0, idx)

        for h in BOTH:
            for kb in BOTH:
                chunk_load(j, slot, h, kb, halves[h]).start()

        @on_stay
        def _():
            for h in BOTH:
                for a in BOTH:
                    chunk_load(j, slot, h, 2 + a, halves[h]).start()

        @on_swap
        def _():
            pltpu.make_async_copy(dyg.at[pl.ds(0, hb)], xg.at[pl.ds(0, hb)], grecv.at[j]).wait()
            for h in BOTH:
                for a in BOTH:
                    chunk_load(j, slot, h, 4 + a, halves[h]).start()

    @scope("chunk")
    def chunk_compute(j):
        slot = lax.rem(j, 2)
        f_a, f_b, _, _ = chunk(j, team, r, t, cx, cy)
        halves = (f_a, f_b)
        for h in BOTH:
            for what in range(4):
                chunk_load(j, slot, h, what, halves[h]).wait()
        for nt in BOTH:
            cols = pl.ds(nt * fh, fh)
            lhs = al(slot * 2 * rb, 2 * rb)
            dh = dot(wb[0, pl.ds(lhs, rb), :], wb[1, pl.ds(nt * fh, fh), :], NT)
            dh += dot(wb[0, pl.ds(lhs + rb, rb), :], wb[1, pl.ds(ff + nt * fh, fh), :], NT)
            g = gu[slot, 0, :, cols].astype(F32)
            u = gu[slot, 1, :, cols].astype(F32)
            sig = jax.nn.sigmoid(g)
            act = g * sig
            d_up = (dh * act).astype(BF16)
            d_gate = ((dh * u) * (sig * (1.0 + g * (1.0 - sig)))).astype(BF16)
            hidden = (act * u).astype(BF16)
            for h in BOTH:
                rows = pl.ds(al(halves[h] * rb + h * hb, hb), hb)
                part = slice(h * hb, (h + 1) * hb)
                dgu[rows, nt * fh : (nt + 1) * fh] = d_gate[part]
                dgu[rows, ff + nt * fh : ff + (nt + 1) * fh] = d_up[part]
                hid[rows, nt * fh : (nt + 1) * fh] = hidden[part]

    chunk_start(0)

    @on_stay
    def _():
        chunk_start(1)

    for kb in BOTH:
        wd_load(wd, kb).wait()

    @pl.loop(0, blocks)
    def _(j):
        chunk_compute(j)
        ring_steps(DURING_CHUNKS, j)

        @pl.when(j + 1 + stay < blocks)
        def _():
            chunk_start(j + 1 + stay)

    half = tok // 2

    def dy_cols(q, slot, th):
        return pltpu.make_async_copy(
            dyg.at[pl.ds(th * half, half), pl.ds(al(q * cq, cq), cq)],
            wb.at[slot, :, pl.ds(th * cq, cq)],
            wsem.at[2 * slot + th],
        )

    def dd_out(i, to):
        ft = lax.rem(i, 4)
        rows = pl.ds(al(ft * rb, rb), rb)
        cols = pl.ds(al((i // 4) * cq, cq), cq)
        return pltpu.make_async_copy(gu.at[ft // 2, lax.rem(ft, 2)], to.at[rows, cols], dsem.at[ft])

    def dd_remote(i):
        ft = lax.rem(i, 4)
        l = ft // 2
        at = (pl.ds(al(ft * rb, rb), rb), pl.ds(al((i // 4) * cq, cq), cq))
        return remote(gu.at[l, lax.rem(ft, 2)], od.at[at], dsem.at[ft], orecv.at[l], pdp, cx * (1 - l) + cy * l)

    def dy_slot(q):
        return (q + 1) // 2 % 2

    def dy_start(q):
        for th in BOTH:
            dy_cols(q, dy_slot(q), th).start()

    @scope("dw_down")
    def down_tile(i, early):
        q = i // 4
        ft = lax.rem(i, 4)
        slot = dy_slot(q)

        @pl.when(ft == 0)
        def _():
            for th in BOTH:
                dy_cols(q, slot, th).wait()

        if not early:
            pl.when(i >= 12)(lambda: dd_out(i - 4, od).wait())
        cols = pl.ds(al(ft * rb, rb), rb)
        o = dot(hid[0:half, cols], wb[slot, :, 0:cq], TN)
        o += dot(hid[half:tok, cols], wb[slot, :, cq : 2 * cq], TN)
        gu[ft // 2, lax.rem(ft, 2)] = o.astype(BF16)

        @on_stay
        def _():
            dd_out(i, od).start()

        @on_swap
        def _():
            (dd_out(i, cwd) if early else dd_remote(i)).start()

    def down_end(q):
        for ft in range(4):
            dd_out(4 * q + ft, od).wait()

        @on_swap
        def _():
            for l in BOTH:
                down_send(l, q).start()

    def w_load(q, a, src):
        rows = pl.ds(al(q * cq, cq), cq)
        slot = lax.rem(q, 2)
        return pltpu.make_async_copy(
            src.at[rows, :], wb.at[0, pl.ds(al(slot * cq, cq), cq), pl.ds(a * ff, ff)], wsem.at[4 + 2 * slot + a]
        )

    @scope("w_start")
    def w_start(q):
        @on_stay
        def _():
            for a in BOTH:
                w_load(q, a, (wg, wu)[a]).start()

        @on_swap
        def _():
            for a in BOTH:
                for l in BOTH:
                    cross_w(q, l, a).wait_recv()
                w_load(q, a, (cwg, cwu)[a]).start()

    dy_start(0)
    dy_start(1)

    for q in BOTH:

        @pl.loop(4 * q, 4 * q + 4)
        def _(i):
            down_tile(i, True)
            ring_steps(DURING_DOWN, i)

        if q:
            w_start(0)
        down_end(q)
    dy_start(2)

    def own_f(i):
        return blk_f(i, i)

    def other_f(i):
        return stay_f(i, team) * swap + swap_f(i, team) * stay

    def xf_out(step):
        q, i, o = step // ring_len, lax.rem(step, ring_len), lax.rem(step, 2)
        rows = pl.ds(al(own_f(i) * rb, rb), rb)
        return pltpu.make_async_copy(xf.at[o], dxp.at[rows, pl.ds(al(q * cq, cq), cq)], xfs.at[o])

    def xb_out(q, i, o):
        rows = pl.ds(al(other_f(i) * rb, rb), rb)
        return remote(out.at[o, 0], dxr.at[rows, pl.ds(al(q * cq, cq), cq)], xbs.at[o], drr.at[q // 2], pdp, t)

    def xb_send(step):
        return xb_out(step // ring_len, lax.rem(step, ring_len), lax.rem(step, 2))

    def rs_nbr(dn):
        return prv * (1 - dn) + nxt * dn

    def rs_send(dn, k, u, slot):
        return remote(rso.at[slot], rsl.at[dn, k, u], rss.at[slot], rsr.at[dn, k, u], dp, rs_nbr(dn))

    def slot_free(slot):
        pltpu.make_async_copy(rso.at[slot], rso.at[slot], rss.at[slot]).wait()

    def rs_part(which, slot, blk, dn, u):
        rows = pl.ds(al(blk * rb + dn * hb, hb), hb)
        cols = pl.ds(al(u * kd, kd), kd)
        src, dst = ((dxp, rpx), (dxr, rpr))[which]
        return pltpu.make_async_copy(src.at[rows, cols], dst.at[slot], rls.at[slot, which])

    def rs_sum(slot, to, received):
        @pl.loop(0, hb // 16)
        def _(i):
            rows = pl.ds(al(i * 16, 16), 16)
            v = rpx[slot, rows, :] + rpr[slot, rows, :].astype(F32)
            if received:
                v += rin[slot, rows, :].astype(F32)
            rso[to, rows, :] = v.astype(BF16)

    @scope("sum_start")
    def rs_start(u):
        all_of_it = pl.ds(0, ring_len * rb // 2)
        pltpu.make_async_copy(dyg.at[all_of_it], dxr.at[all_of_it], drr.at[u]).wait()

        def first(blks, k, base):
            for dn in BOTH:
                for which in BOTH:
                    rs_part(which, dn, blks[dn], dn, u).start()
            for dn in BOTH:
                for which in BOTH:
                    rs_part(which, dn, blks[dn], dn, u).wait()
                slot = base + 2 * u + dn
                rs_sum(dn, slot, False)
                rs_send(dn, k, u, slot).start()

        first((blk_f(r + 1, r + 1), blk_f(r - 1, r + 5)), 0, 0)

        @on_swap
        def _():
            first((swap_f(r - 1, team), swap_f(r - 1, team)), 5, 4)

    def rs_place(tt):
        m = tt // 4
        dn = lax.rem(tt, 2)
        pair = lax.rem(tt // 2, 2)
        early = jnp.where(m < 2, swap, 0)
        k = early * 5 * pair + (1 - early) * (m - swap)
        u = early * m + (1 - early) * pair
        to = 4 * (early * pair + (1 - early) * lax.rem(m, 2)) + 2 * u + dn
        late = jnp.where(k == 5, 1, 0)
        q_stay = (r - 6 + k) * (1 - dn) + (r + 6 - k) * dn
        q_swap = (r - 6 + k + late) * (1 - dn) + (r + 4 - k - late) * dn
        return m, k, u, dn, blk_f(q_stay, q_swap), to

    def rs_in(dn, k, u, slot):
        return pltpu.make_async_copy(rsl.at[dn, k, u], rin.at[slot], rls.at[slot, 2])

    @scope("sum_take")
    def rs_take(tt, slot):
        m, k, u, dn, blk, to = rs_place(tt)

        @pl.when((stay == 1) | (m < 6))
        def _():
            rs_part(0, slot, blk, dn, u).start()
            rs_part(1, slot, blk, dn, u).start()
            rs_send(dn, k, u, 0).wait_recv()
            rs_in(dn, k, u, slot).start()

    def dx_out(dn, u, slot):
        cols = pl.ds(al(u * kd, kd), kd)
        return pltpu.make_async_copy(rso.at[slot], dx.at[pl.ds(al(dn * hb, hb), hb), cols], rss.at[slot])

    def rs_back(l, dn, u, slot):
        return remote(rso.at[slot], crs.at[l, dn, u], rss.at[slot], crr.at[l, dn, u], pdp, cx * (1 - l) + cy * l)

    @scope("sum_give")
    def rs_give(tt, slot):
        m, k, u, dn, blk, to = rs_place(tt)

        @pl.when((stay == 1) | (m < 6))
        def _():
            rs_part(0, slot, blk, dn, u).wait()
            rs_part(1, slot, blk, dn, u).wait()
            rs_in(dn, k, u, slot).wait()

            @pl.when((m != 1) | (swap == 1))
            def _():
                slot_free(to)

            rs_sum(slot, to, True)

            @pl.when(k < 4 + 2 * stay)
            def _():
                rs_send(dn, k + 1, u, to).start()

            @pl.when(k == 6)
            def _():
                dx_out(dn, u, to).start()

            @pl.when((swap == 1) & (k >= 4))
            def _():
                is_r = (k - 4) * (1 - dn) + (5 - k) * dn
                rs_back(lax.rem(is_r + odd, 2), dn, u, to).start()

    @pl.loop(0, 4 * ring_len)
    @scope("dx")
    def _(step):
        q = step // ring_len
        i = lax.rem(step, ring_len)
        o = lax.rem(step, 2)


        @pl.when(i == 0)
        def _():
            for a in BOTH:
                w_load(q, a, wg).wait()

        @pl.when((i == 7) & (q < 3))
        def _():
            w_start(q + 1)

        @pl.when(step >= 2)
        def _():
            xf_out(step - 2).wait()
            xb_send(step - 2).wait_send()

        w = pl.ds(al(lax.rem(q, 2) * cq, cq), cq)
        rows = pl.ds(al(own_f(i) * rb, rb), rb)
        xf[o] = dot(dgu[rows, :], wb[0, w, :], NT)
        xf_out(step).start()
        rows = pl.ds(al(other_f(i) * rb, rb), rb)
        out[o, 0] = dot(dgu[rows, :], wb[0, w, :], NT).astype(BF16)
        xb_send(step).start()
        ring_steps(DURING_DX, step)

    for step in (4 * ring_len - 2, 4 * ring_len - 1):
        xf_out(step).wait()
        xb_send(step).wait_send()

    ring_step(1, 6)
    rs_start(1)
    dy_start(3)
    for i in range(8):
        d2d_wait(1, i)

    def x_cols(i, th):
        slot = lax.rem(i, 4)
        return pltpu.make_async_copy(
            xg.at[pl.ds(th * half, half), pl.ds(al(i * rb, rb), rb)],
            wb.at[1, :, pl.ds(al(slot * 2 * rb + th * rb, rb), rb)],
            wsem.at[(4, 6)[th] + lax.rem(slot, 2) + 4 * (slot // 2)],
        )

    def x_start(i):
        for th in BOTH:
            x_cols(i, th).start()

    def dw_local(i, a):
        o = lax.rem(i, 4)
        return pltpu.make_async_copy(out.at[o, a], (og, ou)[a].at[pl.ds(al(i * rb, rb), rb), :], osem.at[o, a, 0])

    def dw_remote(i, a, l):
        o = lax.rem(i, 4)
        rows = pl.ds(al(i * rb, rb), rb)
        cols = pl.ds(l * fh, fh)
        return remote(out.at[o, a, :, cols], (og, ou)[a].at[rows, cols], osem.at[o, a, l], orecv.at[l], pdp, links[l])

    def dw_start(i, a):
        @on_stay
        def _():
            dw_local(i, a).start()

        @on_swap
        def _():
            for l in BOTH:
                dw_remote(i, a, l).start()

    @scope("dw_wait")
    def dw_wait(i, a):
        @on_stay
        def _():
            dw_local(i, a).wait()

        @on_swap
        def _():
            for l in BOTH:
                dw_remote(i, a, l).wait_send()

    for q in (2, 3):

        @pl.loop(0, 2)
        def _(i):
            tt = 2 * q - 4 + i
            rs_take(tt, 0)
            down_tile(4 * q + 2 * i, False)
            rs_give(tt, 0)
            down_tile(4 * q + 2 * i + 1, False)

        if q == 2:
            for i in range(3):
                x_start(i)

    @pl.loop(0, blocks)
    @scope("dw")
    def _(i):
        o = lax.rem(i, 4)

        @pl.when(i + 3 < blocks)
        def _():
            x_start(i + 3)

        for th in BOTH:
            x_cols(i, th).wait()
        rs_take(4 + i, 0)
        for a in BOTH:

            @pl.when(i >= 4)
            def _():
                dw_wait(i - 4, a)

            cols = slice(a * ff, (a + 1) * ff)
            v = dot(wb[1, :, pl.ds(al(o * 2 * rb, rb), rb)], dgu[0:half, cols], TN)
            v += dot(wb[1, :, pl.ds(al(o * 2 * rb + rb, rb), rb)], dgu[half:tok, cols], TN)
            out[o, a] = v.astype(BF16)
            dw_start(i, a)
            if a == 0:
                rs_give(4 + i, 0)

    @pl.loop(blocks + 4, 28)
    def _(tt):
        rs_take(tt, 0)
        rs_give(tt, 0)

    def sent(sem, rows):
        at = pl.ds(0, rows)
        pltpu.make_async_copy(dyg.at[at], xg.at[at], sem).wait()

    with scope("sent_dw"):
        for i in range(12, 16):
            dd_out(i, od).wait()
        for i in range(blocks - 4, blocks):
            for a in BOTH:
                dw_wait(i, a)
    for a in BOTH:
        sent(dsend.at[a], ring_len * rb)
        on_stay(functools.partial(sent, rsend.at[a], 14 * hb))
        on_swap(functools.partial(sent, rsend.at[a], 12 * hb))

    @on_swap
    @scope("tail")
    def _():
        for l in BOTH:
            sent(csend.at[l], 13 * rb)
            sent(orecv.at[l], 6 * rb)

        def back(dn, u, l):
            return pltpu.make_async_copy(crs.at[l, dn, u], rin.at[l], csem.at[l])

        for u in BOTH:
            for dn in BOTH:
                slot = 2 * u + dn
                for l in BOTH:
                    rs_back(l, dn, u, 0).wait_recv()
                    back(dn, u, l).start()
                for l in BOTH:
                    back(dn, u, l).wait()
                slot_free(slot)

                @pl.loop(0, hb // 16)
                def _(i):
                    rows = pl.ds(al(i * 16, 16), 16)
                    rso[slot, rows, :] = (rin[0, rows, :].astype(F32) + rin[1, rows, :].astype(F32)).astype(BF16)

                dx_out(dn, u, slot).start()

    with scope("slots"):
        for slot in range(8):
            slot_free(slot)


def copy_out(*refs):
    count = len(refs) // 4
    srcs, dsts, bufs, sems = (refs[i * count : (i + 1) * count] for i in range(4))
    moves = []
    for src, dst, buf, sem in zip(srcs, dsts, bufs, sems):
        pieces = sem.shape[1]
        rows = src.shape[0] // pieces
        for i in range(pieces):
            at = pl.ds(i * rows, rows)
            moves.append(
                (
                    pltpu.make_async_copy(src.at[at], buf.at[at], sem.at[0, i]),
                    pltpu.make_async_copy(buf.at[at], dst.at[at], sem.at[1, i]),
                )
            )
    for load, _ in moves:
        load.start()
    for load, store in moves:
        load.wait()
        store.start()
    for _, store in moves:
        store.wait()


def solution(mesh):
    side = math.isqrt(mesh.shape["tp"])

    def local(x, dy, gate, up, wg, wu, wd):
        rb, d = x.shape
        tok, ff = gate.shape
        hb, kd, blocks = rb // 2, d // 2, tok // rb

        def hbm(*shape, dtype=BF16):
            return jax.ShapeDtypeStruct(shape, dtype)

        outs = [
            hbm(rb, d), hbm(d, ff), hbm(d, ff), hbm(ff, d),
            hbm(tok, d), hbm(tok, d),
            hbm(tok, ff), hbm(tok, ff), hbm(d, ff), hbm(d, ff), hbm(ff, d),
            hbm(tok, d, dtype=F32), hbm(tok, d),
            hbm(2, 7, 2, hb, kd), hbm(2, 2, 2, hb, kd),
        ]
        sem = pltpu.SemaphoreType.DMA
        scratch = [
            pltpu.VMEM((tok, 2 * ff), BF16),
            pltpu.VMEM((tok, ff), BF16),
            pltpu.VMEM((2, tok // 2, kd), BF16),
            pltpu.VMEM((2, 2, rb, ff), BF16),
            pltpu.VMEM((4, 2, rb, ff), BF16),
            pltpu.VMEM((2, rb, d // 4), F32),
            pltpu.VMEM((2, hb, kd), BF16),
            pltpu.VMEM((2, hb, kd), F32),
            pltpu.VMEM((2, hb, kd), BF16),
            pltpu.VMEM((8, hb, kd), BF16),
            sem((2,)), sem((2, 2, 7, SUB)), sem((2,)), sem((2, 8)), sem((2,)), sem((2, 11)), sem((blocks,)),
            sem((12,)), sem((2, 2, 4)), sem((4, 2, 2)), sem((2,)),
            sem((2,)), sem((2,)), sem((2,)), sem((8,)), sem((2, 7, 2)), sem((2, 3)), sem((2, 2, 2)), sem((2,)), sem((4,)),
        ]
        res = pl.pallas_call(
            functools.partial(kernel, side),
            out_shape=outs,
            in_specs=[pl.BlockSpec(memory_space=pl.ANY)] * 7,
            out_specs=[pl.BlockSpec(memory_space=pl.ANY)] * len(outs),
            scratch_shapes=scratch,
            compiler_params=pltpu.CompilerParams(
                collective_id=0, has_side_effects=True, vmem_limit_bytes=64 * 2**20 - 2**16
            ),
            name="gated_mlp_backward",
        )(x, dy, gate, up, wg, wu, wd)
        res = res[:4]
        anywhere = [pl.BlockSpec(memory_space=pl.ANY)] * len(res)
        return pl.pallas_call(
            copy_out,
            out_shape=[hbm(*v.shape) for v in res],
            in_specs=anywhere,
            out_specs=anywhere,
            scratch_shapes=[pltpu.VMEM(v.shape, BF16) for v in res]
            + [sem((2, max(1, v.size // (4 * rb * ff)))) for v in res],
            compiler_params=pltpu.CompilerParams(vmem_limit_bytes=48 * 2**20),
            name="copy_out",
        )(*res)

    rows, cols = P(("dp", "tp"), None), P("dp", "tp")
    return jax.shard_map(
        local,
        mesh=mesh,
        in_specs=(rows, rows, cols, cols, P(None, "tp"), P(None, "tp"), P("tp", None)),
        out_specs=(rows, cols, cols, rows),
        check_vma=False,
    )
```

```python
import functools
import math

import jax
import jax.numpy as jnp
from jax import lax
from jax.experimental import pallas as pl
from jax.experimental.pallas import tpu as pltpu
from jax.sharding import PartitionSpec as P

MESH = pl.DeviceIdType.MESH
BF16 = jnp.bfloat16
F32 = jnp.float32
NT = (((1,), (1,)), ((), ()))
TN = (((0,), (0,)), ((), ()))
BOTH = (0, 1)
SUB = 2
PIECES = tuple(range(SUB))

X_AFTER = 9
START = -1
SUMS = -2
NEVER = -1
DURING_CHUNKS = (
    (0, 2, 2, 2), (0, 3, 4, 6), (0, 4, 6, 8), (0, 5, 8, 10), (0, 6, 10, NEVER),
    (1, START, 10, 10), (1, 0, 12, 14),
)
DURING_DOWN = ((1, 1, 3, 5),)
DURING_DX = ((1, 2, 3, 4), (1, 3, 12, 13), (1, 4, 21, 22), (1, 5, 30, 31), (1, SUMS, 31, 23))


scope = jax.named_scope


def parity(v):
    return lax.rem(v, 2)


def dot(a, b, dims):
    return lax.dot_general(a, b, dims, preferred_element_type=F32)


def kernel(
    side,
    x_in, dy_in, gate, up, wg, wu, wd,
    fin0, fin1, rest, og, ou, od, xg, dyg, cg, cu, cwg, cwu, cwd, dxp, dxr, rsl, crs,
    dgu, hid, wb, gu, out, xf, rin, rpx, rpr, rso,
    rsend, rrecv, dsend, drecv, csend, crecv, grecv,
    wsem, lsem, osem, orecv, xfs, xbs, drr, rss, rsr, rls, crr, csem, dsem,
):
    n = side
    ring_len = 2 * n
    rb, d_model = x_in.shape
    tok, ff = gate.shape
    hb = rb // 2
    fh = ff // 2
    kd = d_model // 2
    piece = hb // SUB
    blocks = tok // rb
    cq = d_model // 4

    t = lax.axis_index("tp")
    dp = lax.axis_index("dp")
    c = parity(dp)
    x = t // n
    y = lax.rem(t, n)
    s = lax.rem(x + y, n)
    team = s // 2
    odd = parity(s)
    swap = parity(c + team)
    stay = 1 - swap
    pdp = dp + 1 - 2 * c

    def on_stay(f):
        pl.when(stay == 1)(f)

    def on_swap(f):
        pl.when(swap == 1)(f)

    def wrap(v):
        return lax.rem(v + 2 * n, n)

    def wr(v):
        return lax.rem(v + 4 * ring_len, ring_len)

    def neighbours(x, y, odd):
        sg = 2 * odd - 1
        cx = wrap(x + sg) * n + y
        cy = x * n + wrap(y + sg)
        rx = wrap(x - sg) * n + y
        ry = x * n + wrap(y - sg)
        return cx, cy, rx * (1 - odd) + ry * odd, ry * (1 - odd) + rx * odd

    cx, cy, nxt, prv = neighbours(x, y, odd)
    links = (cx, cy)
    r = wr(2 * x - odd)

    def stay_f(q, team):
        q = wr(q)
        o = parity(q)
        bx = lax.rem((q + o) // 2, n)
        return bx * n + wrap(2 * team + o - bx)

    def swap_f(q, team):
        q = wr(q)
        o = parity(q)
        bx = lax.rem((q + 3 * o) // 2, n)
        return bx * n + wrap(2 * (1 - team) + (1 - o) - bx)

    def blk_f(q_stay, q_swap):
        return stay_f(q_stay, team) * stay + swap_f(q_swap, team) * swap

    def send_blk(dn, i):
        if dn == 0:
            return blk_f(r - i, r - i - (1 if i >= 1 else 0))
        return blk_f(r + i, r - 2 if i == 0 else r - 1 + i)

    def arr_blk(dn, k):
        if dn == 0:
            return blk_f(r - 1 - k, r - 1 if k == 0 else r - 2 - k)
        return blk_f(r + 1 + k, r - 1 if k == 0 else r + k)

    def chunk(j, team, r, t, cx, cy):
        k = jnp.maximum(j - 3, 0) // 2
        sw = jnp.where((j == 1) | (j == 2) | ((j >= 4) & (parity(j) == 0)), 1, 0)
        first = jnp.where(k == 0, 1, 0)
        st_a = jnp.where(j == 0, t, stay_f(r - 1 - k, team))
        st_b = jnp.where(j == 0, t, stay_f(r + 1 + k, team))
        entry = jnp.where(j == 1, cx, cy)
        sw_a = jnp.where(j < 3, entry, swap_f(r - 2 - k + first, team))
        sw_b = jnp.where(j < 3, entry, swap_f(r + k - first, team))
        return sw_a * sw + st_a * (1 - sw), sw_b * sw + st_b * (1 - sw), sw, k

    def al(v, m):
        return pl.multiple_of(v, m)

    bar = pltpu.get_barrier_semaphore()
    peers = ((dp, nxt), (dp, prv), (pdp, t), (pdp, cx), (pdp, cy))
    for p, f in peers:
        pl.semaphore_signal(bar, inc=1, device_id={"dp": p, "tp": f}, device_id_type=MESH)
    pl.semaphore_wait(bar, len(peers))

    ins = (dy_in, x_in)
    gath = (dyg, xg)
    nbr = (nxt, prv)

    def remote(src, dst, ssem, rsem, to_dp, to_tp):
        return pltpu.make_async_remote_copy(
            src, dst, ssem, rsem, device_id={"dp": to_dp, "tp": to_tp}, device_id_type=MESH
        )

    def rows_of(blk, dn, u):
        return pl.ds(al(blk * rb + (dn * hb + u * piece), piece), piece)

    def ring(a, dn, i, u, blk, own=False):
        dst = gath[a].at[rows_of(blk, dn, u)]
        src = ins[a].at[pl.ds(dn * hb + u * piece, piece)] if own else dst
        return remote(src, dst, rsend.at[a], rrecv.at[a, dn, i, u], dp, nbr[dn])

    def d2d(a, dn, i, u, blk, own=False):
        dst = gath[a].at[rows_of(blk, dn, u)]
        src = ins[a].at[pl.ds(dn * hb + u * piece, piece)] if own else dst
        return remote(src, dst, dsend.at[a], drecv.at[a, i], pdp, t)

    def d2d_wait(a, i):
        pltpu.make_async_copy(dyg.at[pl.ds(0, rb)], gath[a].at[pl.ds(0, rb)], drecv.at[a, i]).wait()

    def cross(l, j):
        cols = pl.ds(l * fh, fh)
        if j < 2:
            src, dst = ins[j], gath[j].at[pl.ds(al(t * rb, rb), rb)]
        else:
            src, dst = wd.at[cols], cwd.at[cols]
        return remote(src, dst, csend.at[l], crecv.at[l, j], pdp, links[l])

    def down_send(l, q):
        at = (pl.ds(l * fh, fh), pl.ds(q * cq, cq))
        return remote(cwd.at[at], od.at[at], csend.at[l], orecv.at[l], pdp, links[l])

    def cross_w(q, l, a):
        rows = pl.ds(al(q * cq, cq), cq)
        cols = pl.ds(l * fh, fh)
        src, dst = ((wg, cwg), (wu, cwu))[a]
        return remote(src.at[rows, cols], dst.at[rows, cols], csend.at[l], crecv.at[l, 3 + 2 * q + a], pdp, links[l])

    def cross_gu(l, j, h, a, f):
        rows = pl.ds(al(f * rb + h * hb, hb), hb)
        cols = pl.ds(l * fh, fh)
        src, dst = ((gate, cg), (up, cu))[a]
        return remote(src.at[rows, cols], dst.at[rows, cols], csend.at[l], grecv.at[j], pdp, links[l])

    def their_chunk(l, j):
        f = links[l]
        fx, fy = f // n, lax.rem(f, n)
        f_odd = 1 - odd
        f_cx, f_cy, _, _ = neighbours(fx, fy, f_odd)
        f_a, f_b, _, _ = chunk(j, 1 - team, wr(2 * fx - f_odd), f, f_cx, f_cy)
        return f_a, f_b

    def cross_chunks(lo, hi):
        @pl.loop(lo, hi)
        def _(j):
            for l in BOTH:
                halves = their_chunk(l, j)
                for h in BOTH:
                    for a in BOTH:
                        cross_gu(l, j, h, a, halves[h]).start()

    @scope("ring_start")
    def ring_start(a):
        @on_stay
        def _():
            for u in PIECES:
                for dn in BOTH:
                    ring(a, dn, 0, u, t, own=True).start()
            for u in PIECES:
                for dn in BOTH:
                    d2d(a, dn, 7, u, t, own=True).start()

        @on_swap
        def _():
            for l in BOTH:
                cross(l, a).wait_recv()
            for i in BOTH:
                for u in PIECES:
                    for dn in BOTH:
                        ring(a, dn, i, u, send_blk(dn, i)).start()
            for l in BOTH:
                for u in PIECES:
                    for dn in BOTH:
                        d2d(a, dn, 6 + l, u, links[l]).start()

    def ring_step(a, k):
        def body():
            for u in PIECES:
                for dn in BOTH:
                    b = arr_blk(dn, k)
                    ring(a, dn, k, u, b).wait_recv()

                    def forward():
                        ring(a, dn, k + 1, u, b).start()

                    if 1 <= k <= 4:
                        forward()
                    elif k < 6:
                        on_stay(forward)
                    d2d(a, dn, k, u, b).start()

        with scope(f"ring_{a}_{k}"):
            if k == 6:
                on_stay(body)
            else:
                body()

    def ring_steps(table, i):
        for a, k, on_stay_at, on_swap_at in table:

            @pl.when(i == on_stay_at * stay + on_swap_at * swap)
            def _():
                if k == SUMS:
                    rs_start(0)
                elif k == START:
                    ring_start(a)
                else:
                    ring_step(a, k)

    def bounce(a, h, kb, out_):
        vm = dgu.at[pl.ds((2 * a + kb) * rb + h * hb, hb), :]
        cols = pl.ds(kb * kd, kd)
        if out_:
            return pltpu.make_async_copy(vm, gath[a].at[pl.ds(al(t * rb + h * hb, hb), hb), cols], lsem.at[0, h, 2 * a + kb])
        return pltpu.make_async_copy(ins[a].at[pl.ds(h * hb, hb), cols], vm, lsem.at[0, h, 2 * a + kb])

    def wd_load(src, kb):
        return pltpu.make_async_copy(src.at[:, pl.ds(kb * kd, kd)], wb.at[1, pl.ds(kb * ff, ff), :], wsem.at[kb])

    early = blocks // 2

    @on_swap
    def _():
        for j in (0, 2):
            for l in BOTH:
                cross(l, j).start()
        cross_chunks(0, early)

    @on_stay
    def _():
        for a in BOTH:
            for h in BOTH:
                for kb in BOTH:
                    bounce(a, h, kb, False).start()
        for kb in BOTH:
            wd_load(wd, kb).start()

    ring_start(0)

    @on_stay
    def _():
        for out_ in (False, True):
            for a in BOTH:
                for h in BOTH:
                    for kb in BOTH:
                        bounce(a, h, kb, out_).wait()
                        if not out_:
                            bounce(a, h, kb, True).start()

    ring_step(0, 0)

    @on_swap
    def _():
        cross_chunks(early, X_AFTER)
        for l in BOTH:
            cross(l, 1).start()
        cross_chunks(X_AFTER, blocks)

        @pl.loop(0, 4)
        def _(q):
            for a in BOTH:
                for l in BOTH:
                    cross_w(q, l, a).start()

    ring_step(0, 1)

    @on_swap
    def _():
        for l in BOTH:
            cross(l, 2).wait_recv()
        for kb in BOTH:
            wd_load(cwd, kb).start()

    def chunk_load(j, slot, h, what, f):
        rows = pl.ds(al(f * rb + h * hb, hb), hb)
        sem = lsem.at[slot, h, what]
        if what < 2:
            dst = wb.at[0, pl.ds(al(slot * 2 * rb + what * rb + h * hb, hb), hb), :]
            return pltpu.make_async_copy(dyg.at[rows, pl.ds(what * kd, kd)], dst, sem)
        dst = gu.at[slot, what % 2, pl.ds(h * hb, hb), :]
        src = ((gate, up), (cg, cu))[what // 4][what % 2]
        return pltpu.make_async_copy(src.at[rows, :], dst, lsem.at[slot, h, 2 + what % 2])

    @scope("chunk_start")
    def chunk_start(j):
        slot = parity(j)
        f_a, f_b, sw, k = chunk(j, team, r, t, cx, cy)
        halves = (f_a, f_b)

        @pl.when(sw != swap)
        def _():
            idx = jnp.where(j == 0, 7, jnp.where(j < 3, 5 + j, k))
            d2d_wait(0, idx)

        for h in BOTH:
            for kb in BOTH:
                chunk_load(j, slot, h, kb, halves[h]).start()

        @on_stay
        def _():
            for h in BOTH:
                for a in BOTH:
                    chunk_load(j, slot, h, 2 + a, halves[h]).start()

        @on_swap
        def _():
            pltpu.make_async_copy(dyg.at[pl.ds(0, hb)], xg.at[pl.ds(0, hb)], grecv.at[j]).wait()
            for h in BOTH:
                for a in BOTH:
                    chunk_load(j, slot, h, 4 + a, halves[h]).start()

    @scope("chunk")
    def chunk_compute(j):
        slot = parity(j)
        f_a, f_b, _, _ = chunk(j, team, r, t, cx, cy)
        halves = (f_a, f_b)
        for h in BOTH:
            for what in range(4):
                chunk_load(j, slot, h, what, halves[h]).wait()
        for nt in BOTH:
            cols = pl.ds(nt * fh, fh)
            lhs = al(slot * 2 * rb, 2 * rb)
            dh = dot(wb[0, pl.ds(lhs, rb), :], wb[1, pl.ds(nt * fh, fh), :], NT)
            dh += dot(wb[0, pl.ds(lhs + rb, rb), :], wb[1, pl.ds(ff + nt * fh, fh), :], NT)
            g = gu[slot, 0, :, cols].astype(F32)
            u = gu[slot, 1, :, cols].astype(F32)
            sig = jax.nn.sigmoid(g)
            act = g * sig
            d_up = (dh * act).astype(BF16)
            d_gate = ((dh * u) * (sig * (1.0 + g * (1.0 - sig)))).astype(BF16)
            hidden = (act * u).astype(BF16)
            for h in BOTH:
                rows = pl.ds(al(halves[h] * rb + h * hb, hb), hb)
                part = slice(h * hb, (h + 1) * hb)
                dgu[rows, nt * fh : (nt + 1) * fh] = d_gate[part]
                dgu[rows, ff + nt * fh : ff + (nt + 1) * fh] = d_up[part]
                hid[rows, nt * fh : (nt + 1) * fh] = hidden[part]

    chunk_start(0)

    @on_stay
    def _():
        chunk_start(1)

    for kb in BOTH:
        wd_load(wd, kb).wait()

    @pl.loop(0, blocks)
    def _(j):
        chunk_compute(j)
        ring_steps(DURING_CHUNKS, j)

        @pl.when(j + 1 + stay < blocks)
        def _():
            chunk_start(j + 1 + stay)

    half = tok // 2

    def dy_cols(q, slot, th):
        return pltpu.make_async_copy(
            dyg.at[pl.ds(th * half, half), pl.ds(al(q * cq, cq), cq)],
            wb.at[slot, :, pl.ds(th * cq, cq)],
            wsem.at[2 * slot + th],
        )

    def down_rows(i):
        return 2 * parity(i) + lax.rem(i, 4) // 2

    def dd_out(i, to):
        ft = down_rows(i)
        rows = pl.ds(al(ft * rb, rb), rb)
        cols = pl.ds(al((i // 4) * cq, cq), cq)
        return pltpu.make_async_copy(gu.at[ft // 2, parity(ft)], to.at[rows, cols], dsem.at[ft])

    def dd_remote(i):
        ft = down_rows(i)
        l = ft // 2
        at = (pl.ds(al(ft * rb, rb), rb), pl.ds(al((i // 4) * cq, cq), cq))
        return remote(gu.at[l, parity(ft)], od.at[at], dsem.at[ft], orecv.at[l], pdp, cx * (1 - l) + cy * l)

    def dy_start(q):
        for th in BOTH:
            dy_cols(q, q % 2, th).start()

    @scope("dw_down")
    def down_tile(i, early):
        q = i // 4
        ft = down_rows(i)
        slot = parity(q)

        @pl.when(lax.rem(i, 4) == 0)
        def _():
            for th in BOTH:
                dy_cols(q, slot, th).wait()

        if not early:
            pl.when(i >= 12)(lambda: dd_out(i - 4, od).wait())
        cols = pl.ds(al(ft * rb, rb), rb)
        o = dot(hid[0:half, cols], wb[slot, :, 0:cq], TN)
        o += dot(hid[half:tok, cols], wb[slot, :, cq : 2 * cq], TN)
        gu[ft // 2, parity(ft)] = o.astype(BF16)

        @on_stay
        def _():
            dd_out(i, od).start()

        @on_swap
        def _():
            (dd_out(i, cwd) if early else dd_remote(i)).start()

    def down_end(q):
        for ft in range(4):
            dd_out(4 * q + ft, od).wait()

        @on_swap
        def _():
            for l in BOTH:
                down_send(l, q).start()

    def w_load(q, a, src):
        rows = pl.ds(al(q * cq, cq), cq)
        slot = parity(q)
        return pltpu.make_async_copy(
            src.at[rows, :], wb.at[1, pl.ds(al(slot * cq, cq), cq), pl.ds(a * ff, ff)], wsem.at[4 + 2 * slot + a]
        )

    @scope("w_start")
    def w_start(q):
        @on_stay
        def _():
            for a in BOTH:
                w_load(q, a, (wg, wu)[a]).start()

        @on_swap
        def _():
            for a in BOTH:
                for l in BOTH:
                    cross_w(q, l, a).wait_recv()
                w_load(q, a, (cwg, cwu)[a]).start()

    dy_start(0)
    dy_start(1)

    for q in BOTH:

        @pl.loop(4 * q, 4 * q + 4)
        def _(i):
            down_tile(i, True)
            ring_steps(DURING_DOWN, i)

        down_end(q)
        dy_start(2) if q == 0 else w_start(0)

    @pl.loop(8, 10)
    def _(i):
        down_tile(i, False)

    def own_f(i):
        return blk_f(i, i)

    def other_f(i):
        return stay_f(i, team) * swap + swap_f(i, team) * stay

    def xf_out(step):
        q, i, o = step // ring_len, lax.rem(step, ring_len), parity(step)
        rows = pl.ds(al(own_f(i) * rb, rb), rb)
        return pltpu.make_async_copy(xf.at[o], dxp.at[rows, pl.ds(al(q * cq, cq), cq)], xfs.at[o])

    def xb_out(q, i, o):
        rows = pl.ds(al(other_f(i) * rb, rb), rb)
        return remote(out.at[o, 0], dxr.at[rows, pl.ds(al(q * cq, cq), cq)], xbs.at[o], drr.at[q // 2], pdp, t)

    def xb_send(step):
        return xb_out(step // ring_len, lax.rem(step, ring_len), parity(step))

    def rs_nbr(dn):
        return prv * (1 - dn) + nxt * dn

    def rs_send(dn, k, u, slot):
        return remote(rso.at[slot], rsl.at[dn, k, u], rss.at[slot], rsr.at[dn, k, u], dp, rs_nbr(dn))

    def slot_free(slot):
        pltpu.make_async_copy(rso.at[slot], rso.at[slot], rss.at[slot]).wait()

    def rs_part(which, slot, blk, dn, u):
        rows = pl.ds(al(blk * rb + dn * hb, hb), hb)
        cols = pl.ds(al(u * kd, kd), kd)
        src, dst = ((dxp, rpx), (dxr, rpr))[which]
        return pltpu.make_async_copy(src.at[rows, cols], dst.at[slot], rls.at[slot, which])

    def rs_sum(slot, to, received):
        @pl.loop(0, hb // 16)
        def _(i):
            rows = pl.ds(al(i * 16, 16), 16)
            v = rpx[slot, rows, :] + rpr[slot, rows, :].astype(F32)
            if received:
                v += rin[slot, rows, :].astype(F32)
            rso[to, rows, :] = v.astype(BF16)

    @scope("sum_start")
    def rs_start(u):
        all_of_it = pl.ds(0, ring_len * rb // 2)
        pltpu.make_async_copy(dyg.at[all_of_it], dxr.at[all_of_it], drr.at[u]).wait()

        def first(blks, k, base):
            for dn in BOTH:
                for which in BOTH:
                    rs_part(which, dn, blks[dn], dn, u).start()
            for dn in BOTH:
                for which in BOTH:
                    rs_part(which, dn, blks[dn], dn, u).wait()
                slot = base + 2 * u + dn
                rs_sum(dn, slot, False)
                rs_send(dn, k, u, slot).start()

        first((blk_f(r + 1, r + 1), blk_f(r - 1, r + 5)), 0, 0)

        @on_swap
        def _():
            first((swap_f(r - 1, team), swap_f(r - 1, team)), 5, 4)

    def rs_place(tt):
        m = tt // 4
        dn = parity(tt)
        pair = parity(tt // 2)
        early = jnp.where(m < 2, swap, 0)
        k = early * 5 * pair + (1 - early) * (m - swap)
        u = early * m + (1 - early) * pair
        to = 4 * (early * pair + (1 - early) * parity(m)) + 2 * u + dn
        late = jnp.where(k == 5, 1, 0)
        q_stay = (r - 6 + k) * (1 - dn) + (r + 6 - k) * dn
        q_swap = (r - 6 + k + late) * (1 - dn) + (r + 4 - k - late) * dn
        return m, k, u, dn, blk_f(q_stay, q_swap), to

    def rs_in(dn, k, u, slot):
        return pltpu.make_async_copy(rsl.at[dn, k, u], rin.at[slot], rls.at[slot, 2])

    @scope("sum_take")
    def rs_take(tt, slot):
        m, k, u, dn, blk, to = rs_place(tt)
        rs_part(0, slot, blk, dn, u).start()
        rs_part(1, slot, blk, dn, u).start()
        rs_send(dn, k, u, 0).wait_recv()
        rs_in(dn, k, u, slot).start()

    def last_sum(dn, u, slot):
        return pltpu.make_async_copy(rso.at[slot], (fin0, fin1)[dn].at[:, pl.ds(al(u * kd, kd), kd)], rss.at[slot])

    def rs_back(l, dn, u, slot):
        return remote(rso.at[slot], crs.at[l, dn, u], rss.at[slot], crr.at[l, dn, u], pdp, cx * (1 - l) + cy * l)

    @scope("sum_give")
    def rs_give(tt, slot):
        m, k, u, dn, blk, to = rs_place(tt)
        rs_part(0, slot, blk, dn, u).wait()
        rs_part(1, slot, blk, dn, u).wait()
        rs_in(dn, k, u, slot).wait()

        @pl.when((m != 1) | (swap == 1))
        def _():
            slot_free(to)

        rs_sum(slot, to, True)

        @pl.when(k < 4 + stay)
        def _():
            rs_send(dn, k + 1, u, to).start()

        for half_of in BOTH:

            @pl.when((k == 4 + stay) & (dn == half_of))
            def _():
                last_sum(half_of, u, to).start()

        @pl.when((swap == 1) & (k == 5))
        def _():
            rs_back(parity(1 - dn + odd), dn, u, to).start()

    def rest_put(dn, u):
        blk = t

        @on_stay
        def _():
            for which in BOTH:
                rs_part(which, 1, blk, dn, u).start()
            for which in BOTH:
                rs_part(which, 1, blk, dn, u).wait()

        @on_swap
        def _():
            l = parity(dn + odd)
            rs_back(l, dn, u, 0).wait_recv()
            back = pltpu.make_async_copy(crs.at[l, dn, u], rin.at[1], csem.at[0])
            back.start()
            back.wait()

        @pl.loop(0, hb // 16)
        def _(i):
            rows = pl.ds(al(i * 16, 16), 16)

            @on_stay
            def _():
                rpx[1, rows, :] += rpr[1, rows, :].astype(F32)

            @on_swap
            def _():
                rpx[1, rows, :] = rin[1, rows, :].astype(F32)

        at = (pl.ds(al(dn * hb, hb), hb), pl.ds(al(u * kd, kd), kd))
        leave = pltpu.make_async_copy(rpx.at[1], rest.at[at], csem.at[1])
        leave.start()
        leave.wait()

    @pl.loop(0, 4 * ring_len)
    @scope("dx")
    def _(step):
        q = step // ring_len
        i = lax.rem(step, ring_len)
        o = parity(step)


        @pl.when(i == 0)
        def _():
            for a in BOTH:
                w_load(q, a, wg).wait()

        @pl.when((i == 7) & (q < 3))
        def _():
            w_start(q + 1)

        @pl.when(step >= 2)
        def _():
            xf_out(step - 2).wait()
            xb_send(step - 2).wait_send()

        w = pl.ds(al(parity(q) * cq, cq), cq)
        rows = pl.ds(al(own_f(i) * rb, rb), rb)
        xf[o] = dot(dgu[rows, :], wb[1, w, :], NT)
        xf_out(step).start()
        rows = pl.ds(al(other_f(i) * rb, rb), rb)
        out[o, 0] = dot(dgu[rows, :], wb[1, w, :], NT).astype(BF16)
        xb_send(step).start()
        ring_steps(DURING_DX, step)

    for step in (4 * ring_len - 2, 4 * ring_len - 1):
        xf_out(step).wait()
        xb_send(step).wait_send()

    ring_step(1, 6)
    rs_start(1)
    dy_start(3)
    for i in range(8):
        d2d_wait(1, i)

    def x_cols(i, th):
        slot = lax.rem(i, 4)
        return pltpu.make_async_copy(
            xg.at[pl.ds(th * half, half), pl.ds(al(i * rb, rb), rb)],
            wb.at[0, :, pl.ds(al(slot * 2 * rb + th * rb, rb), rb)],
            wsem.at[(4, 6)[th] + parity(slot) + 4 * (slot // 2)],
        )

    def x_start(i):
        for th in BOTH:
            x_cols(i, th).start()

    def dw_local(i, a):
        o = lax.rem(i, 4)
        return pltpu.make_async_copy(out.at[o, a], (og, ou)[a].at[pl.ds(al(i * rb, rb), rb), :], osem.at[o, a, 0])

    def dw_remote(i, a, l):
        o = lax.rem(i, 4)
        rows = pl.ds(al(i * rb, rb), rb)
        cols = pl.ds(l * fh, fh)
        return remote(out.at[o, a, :, cols], (og, ou)[a].at[rows, cols], osem.at[o, a, l], orecv.at[l], pdp, links[l])

    def dw_start(i, a):
        @on_stay
        def _():
            dw_local(i, a).start()

        @on_swap
        def _():
            for l in BOTH:
                dw_remote(i, a, l).start()

    @scope("dw_wait")
    def dw_wait(i, a):
        @on_stay
        def _():
            dw_local(i, a).wait()

        @on_swap
        def _():
            for l in BOTH:
                dw_remote(i, a, l).wait_send()

    @on_stay
    def _():
        @pl.loop(0, 4)
        def _(i):
            rest_put(parity(i), i // 2)

    @pl.loop(0, 3)
    def _(tt):
        rs_take(tt, 0)
        down_tile(10 + 2 * tt, False)
        rs_give(tt, 0)
        down_tile(11 + 2 * tt, False)
        x_start(tt)

    @pl.loop(0, blocks)
    @scope("dw")
    def _(i):
        o = lax.rem(i, 4)

        @pl.when(i + 3 < blocks)
        def _():
            x_start(i + 3)

        for th in BOTH:
            x_cols(i, th).wait()
        rs_take(3 + i, 0)
        for a in BOTH:

            @pl.when(i >= 4)
            def _():
                dw_wait(i - 4, a)

            cols = slice(a * ff, (a + 1) * ff)
            v = dot(wb[0, :, pl.ds(al(o * 2 * rb, rb), rb)], dgu[0:half, cols], TN)
            v += dot(wb[0, :, pl.ds(al(o * 2 * rb + rb, rb), rb)], dgu[half:tok, cols], TN)
            out[o, a] = v.astype(BF16)
            dw_start(i, a)
            if a == 0:
                rs_give(3 + i, 0)

    first, last = blocks + 3, 24

    @pl.loop(first, last)
    def _(tt):
        @pl.when((swap == 1) & (tt + 1 < last))
        def _():
            rest_put(parity(tt - first), (tt - first) // 2)

        rs_take(tt, 0)
        rs_give(tt, 0)

    def sent(sem, rows):
        at = pl.ds(0, rows)
        pltpu.make_async_copy(dyg.at[at], xg.at[at], sem).wait()

    with scope("sent_dw"):
        for i in range(12, 16):
            dd_out(i, od).wait()
        for i in range(blocks - 4, blocks):
            for a in BOTH:
                dw_wait(i, a)
    for a in BOTH:
        sent(dsend.at[a], ring_len * rb)
        on_stay(functools.partial(sent, rsend.at[a], 14 * hb))
        on_swap(functools.partial(sent, rsend.at[a], 12 * hb))

    @on_swap
    @scope("tail")
    def _():
        for l in BOTH:
            sent(csend.at[l], 13 * rb)
            sent(orecv.at[l], 6 * rb)

    with scope("slots"):
        for slot in range(8):
            slot_free(slot)


def last_hops(groups, n):
    ways = ([], [])
    for dp in range(groups):
        for t in range(n * n):
            x, y = divmod(t, n)
            team, odd = divmod((x + y) % n, 2)
            swap = (dp + team) % 2
            sg = odd if swap else 1 - odd
            step = 2 * sg - 1
            across, along = ((x + step) % n) * n + y, x * n + (y + step) % n
            to = (along, across) if odd else (across, along)
            if not swap:
                to = to[::-1]
            to_dp = dp + 1 - 2 * (dp % 2) if swap else dp
            for way, f in zip(ways, to):
                way.append((dp * n * n + t, to_dp * n * n + f))
    return ways


def copy_out(*refs):
    count = len(refs) // 4
    srcs, dsts, bufs, sems = (refs[i * count : (i + 1) * count] for i in range(4))
    moves = []
    for src, dst, buf, sem in zip(srcs, dsts, bufs, sems):
        pieces = sem.shape[1]
        rows = src.shape[0] // pieces
        for i in range(pieces):
            at = pl.ds(i * rows, rows)
            moves.append(
                (
                    pltpu.make_async_copy(src.at[at], buf.at[at], sem.at[0, i]),
                    pltpu.make_async_copy(buf.at[at], dst.at[at], sem.at[1, i]),
                )
            )
    for load, _ in moves:
        load.start()
    for load, store in moves:
        load.wait()
        store.start()
    for _, store in moves:
        store.wait()


def solution(mesh):
    side = math.isqrt(mesh.shape["tp"])
    ways = last_hops(mesh.shape["dp"], side)

    def local(x, dy, gate, up, wg, wu, wd):
        rb, d = x.shape
        tok, ff = gate.shape
        hb, kd, blocks = rb // 2, d // 2, tok // rb

        def hbm(*shape, dtype=BF16):
            return jax.ShapeDtypeStruct(shape, dtype)

        outs = [
            hbm(hb, d), hbm(hb, d), hbm(rb, d, dtype=F32),
            hbm(d, ff), hbm(d, ff), hbm(ff, d),
            hbm(tok, d), hbm(tok, d),
            hbm(tok, ff), hbm(tok, ff), hbm(d, ff), hbm(d, ff), hbm(ff, d),
            hbm(tok, d, dtype=F32), hbm(tok, d),
            hbm(2, 6, 2, hb, kd), hbm(2, 2, 2, hb, kd),
        ]
        sem = pltpu.SemaphoreType.DMA
        scratch = [
            pltpu.VMEM((tok, 2 * ff), BF16),
            pltpu.VMEM((tok, ff), BF16),
            pltpu.VMEM((2, tok // 2, kd), BF16),
            pltpu.VMEM((2, 2, rb, ff), BF16),
            pltpu.VMEM((4, 2, rb, ff), BF16),
            pltpu.VMEM((2, rb, d // 4), F32),
            pltpu.VMEM((2, hb, kd), BF16),
            pltpu.VMEM((2, hb, kd), F32),
            pltpu.VMEM((2, hb, kd), BF16),
            pltpu.VMEM((8, hb, kd), BF16),
            sem((2,)), sem((2, 2, 7, SUB)), sem((2,)), sem((2, 8)), sem((2,)), sem((2, 11)), sem((blocks,)),
            sem((12,)), sem((2, 2, 4)), sem((4, 2, 2)), sem((2,)),
            sem((2,)), sem((2,)), sem((2,)), sem((8,)), sem((2, 6, 2)), sem((2, 3)), sem((2, 2, 2)), sem((2,)), sem((4,)),
        ]
        res = pl.pallas_call(
            functools.partial(kernel, side),
            out_shape=outs,
            in_specs=[pl.BlockSpec(memory_space=pl.ANY)] * 7,
            out_specs=[pl.BlockSpec(memory_space=pl.ANY)] * len(outs),
            scratch_shapes=scratch,
            compiler_params=pltpu.CompilerParams(
                collective_id=0, has_side_effects=True, vmem_limit_bytes=64 * 2**20 - 2**16
            ),
            name="gated_mlp_backward",
        )(x, dy, gate, up, wg, wu, wd)
        fins, rest, res = res[:2], res[2], res[3:6]
        moved = [lax.ppermute(v, ("dp", "tp"), way) for v, way in zip(fins, ways)]
        anywhere = [pl.BlockSpec(memory_space=pl.ANY)] * len(res)
        grads = pl.pallas_call(
            copy_out,
            out_shape=[hbm(*v.shape) for v in res],
            in_specs=anywhere,
            out_specs=anywhere,
            scratch_shapes=[pltpu.VMEM(v.shape, BF16) for v in res]
            + [sem((2, max(1, v.size // (4 * rb * ff)))) for v in res],
            compiler_params=pltpu.CompilerParams(vmem_limit_bytes=48 * 2**20),
            cost_estimate=pl.CostEstimate(flops=10**10, bytes_accessed=6 * d * ff * 2, transcendentals=0),
            name="copy_out",
        )(*res)
        dx = (jnp.concatenate(moved).astype(F32) + rest).astype(BF16)
        return dx, *grads

    rows, cols = P(("dp", "tp"), None), P("dp", "tp")
    return jax.shard_map(
        local,
        mesh=mesh,
        in_specs=(rows, rows, cols, cols, P(None, "tp"), P(None, "tp"), P("tp", None)),
        out_specs=(rows, cols, cols, rows),
        check_vma=False,
    )
```

```python
import functools
import math

import jax
import jax.numpy as jnp
from jax import lax
from jax.experimental import pallas as pl
from jax.experimental.pallas import tpu as pltpu
from jax.sharding import PartitionSpec as P

MESH = pl.DeviceIdType.MESH
BF16 = jnp.bfloat16
F32 = jnp.float32
NT = (((1,), (1,)), ((), ()))
TN = (((0,), (0,)), ((), ()))
BOTH = (0, 1)
LATE = (2, 3)
FOUR = range(4)
SUB = 2
PIECES = tuple(range(SUB))

X_AFTER = 9
NEVER = -1
DOWN, TERMS, DONE = 16, 24, 56
DY_AT = ((2, 4, 6, 8, 10), (2, 6, 8, 10, NEVER))
X_START = (10, 10)
X_AT = (
    (12, 12, 16, 18, 23, 27, 32, 36, 41, 45, 50, 55),
    (13, 15, 18, 21, 25, 30, 34, 38, 43, 48, 52, 55),
)
SUMS_AT = (55, 49)


scope = jax.named_scope


def parity(v):
    return lax.rem(v, 2)


def dot(a, b, dims):
    return lax.dot_general(a, b, dims, preferred_element_type=F32)


def kernel(
    side,
    x_in, dy_in, gate, up, wg, wu, wd,
    fin0, fin1, rest, short, og, ou, od, xg, dyg, cg, cu, cwg, cwu, cwd, dxp, dxr, rsl, hidr,
    dgu, hid, wb, gu, out, xf, rin, rpx, rpr, rso, hv,
    rsend, rrecv, dsend, drecv, csend, crecv, grecv,
    wsem, lsem, osem, orecv, xfs, xbs, drr, rss, rsr, rls, crr, csem, dsem, hsem,
):
    n = side
    ring_len = 2 * n
    rb, d_model = x_in.shape
    tok, ff = gate.shape
    hb = rb // 2
    fh = ff // 2
    kd = d_model // 2
    piece = hb // SUB
    blocks = tok // rb
    cq = d_model // 4

    t = lax.axis_index("tp")
    dp = lax.axis_index("dp")
    c = parity(dp)
    x = t // n
    y = lax.rem(t, n)
    s = lax.rem(x + y, n)
    team = s // 2
    odd = parity(s)
    swap = parity(c + team)
    stay = 1 - swap
    pdp = dp + 1 - 2 * c

    def on_stay(f):
        pl.when(stay == 1)(f)

    def on_swap(f):
        pl.when(swap == 1)(f)

    def wrap(v):
        return lax.rem(v + 2 * n, n)

    def wr(v):
        return lax.rem(v + 4 * ring_len, ring_len)

    def neighbours(x, y, odd):
        sg = 2 * odd - 1
        cx = wrap(x + sg) * n + y
        cy = x * n + wrap(y + sg)
        rx = wrap(x - sg) * n + y
        ry = x * n + wrap(y - sg)
        return cx, cy, rx * (1 - odd) + ry * odd, ry * (1 - odd) + rx * odd

    cx, cy, nxt, prv = neighbours(x, y, odd)
    links = (cx, cy)
    r = wr(2 * x - odd)

    def stay_f(q, team):
        q = wr(q)
        o = parity(q)
        bx = lax.rem((q + o) // 2, n)
        return bx * n + wrap(2 * team + o - bx)

    def swap_f(q, team):
        q = wr(q)
        o = parity(q)
        bx = lax.rem((q + 3 * o) // 2, n)
        return bx * n + wrap(2 * (1 - team) + (1 - o) - bx)

    def blk_f(q_stay, q_swap):
        return stay_f(q_stay, team) * stay + swap_f(q_swap, team) * swap

    def send_blk(dn, i):
        if dn == 0:
            return blk_f(r - i, r - i - (1 if i >= 1 else 0))
        return blk_f(r + i, r - 2 if i == 0 else r - 1 + i)

    def arr_blk(dn, k):
        if dn == 0:
            return blk_f(r - 1 - k, r - 1 if k == 0 else r - 2 - k)
        return blk_f(r + 1 + k, r - 1 if k == 0 else r + k)

    def chunk(j, team, r, t, cx, cy):
        k = jnp.maximum(j - 3, 0) // 2
        sw = jnp.where((j == 1) | (j == 2) | ((j >= 4) & (parity(j) == 0)), 1, 0)
        first = jnp.where(k == 0, 1, 0)
        st_a = jnp.where(j == 0, t, stay_f(r - 1 - k, team))
        st_b = jnp.where(j == 0, t, stay_f(r + 1 + k, team))
        entry = jnp.where(j == 1, cx, cy)
        sw_a = jnp.where(j < 3, entry, swap_f(r - 2 - k + first, team))
        sw_b = jnp.where(j < 3, entry, swap_f(r + k - first, team))
        return sw_a * sw + st_a * (1 - sw), sw_b * sw + st_b * (1 - sw), sw, k

    def al(v, m):
        return pl.multiple_of(v, m)

    bar = pltpu.get_barrier_semaphore()
    peers = ((dp, nxt), (dp, prv), (pdp, t), (pdp, cx), (pdp, cy), (dp, cx), (dp, cy))
    for p, f in peers:
        pl.semaphore_signal(bar, inc=1, device_id={"dp": p, "tp": f}, device_id_type=MESH)
    pl.semaphore_wait(bar, len(peers))

    ins = (dy_in, x_in)
    gath = (dyg, xg)
    nbr = (nxt, prv)

    def remote(src, dst, ssem, rsem, to_dp, to_tp):
        return pltpu.make_async_remote_copy(
            src, dst, ssem, rsem, device_id={"dp": to_dp, "tp": to_tp}, device_id_type=MESH
        )

    def rows_of(blk, dn, u):
        return pl.ds(al(blk * rb + (dn * hb + u * piece), piece), piece)

    def ring(a, dn, i, u, blk, own=False):
        dst = gath[a].at[rows_of(blk, dn, u)]
        src = ins[a].at[pl.ds(dn * hb + u * piece, piece)] if own else dst
        return remote(src, dst, rsend.at[a], rrecv.at[a, dn, i, u], dp, nbr[dn])

    def d2d(a, dn, i, u, blk, own=False):
        dst = gath[a].at[rows_of(blk, dn, u)]
        src = ins[a].at[pl.ds(dn * hb + u * piece, piece)] if own else dst
        return remote(src, dst, dsend.at[a], drecv.at[a, i], pdp, t)

    def d2d_wait(a, i):
        pltpu.make_async_copy(dyg.at[pl.ds(0, rb)], gath[a].at[pl.ds(0, rb)], drecv.at[a, i]).wait()

    def cross(l, j):
        cols = pl.ds(l * fh, fh)
        if j < 2:
            src, dst = ins[j], gath[j].at[pl.ds(al(t * rb, rb), rb)]
        else:
            src, dst = wd.at[cols], cwd.at[cols]
        return remote(src, dst, csend.at[l], crecv.at[l, j], pdp, links[l])

    def down_send(l, q):
        at = (pl.ds(l * fh, fh), pl.ds(q * cq, cq))
        return remote(cwd.at[at], od.at[at], csend.at[l], orecv.at[l], pdp, links[l])

    def cross_w(q, l, a):
        rows = pl.ds(al(q * cq, cq), cq)
        cols = pl.ds(l * fh, fh)
        src, dst = ((wg, cwg), (wu, cwu))[a]
        return remote(src.at[rows, cols], dst.at[rows, cols], csend.at[l], crecv.at[l, 3 + 2 * q + a], pdp, links[l])

    def cross_gu(l, j, h, a, f):
        rows = pl.ds(al(f * rb + h * hb, hb), hb)
        cols = pl.ds(l * fh, fh)
        src, dst = ((gate, cg), (up, cu))[a]
        return remote(src.at[rows, cols], dst.at[rows, cols], csend.at[l], grecv.at[j], pdp, links[l])

    def their_chunk(l, j):
        f = links[l]
        fx, fy = f // n, lax.rem(f, n)
        f_odd = 1 - odd
        f_cx, f_cy, _, _ = neighbours(fx, fy, f_odd)
        f_a, f_b, _, _ = chunk(j, 1 - team, wr(2 * fx - f_odd), f, f_cx, f_cy)
        return f_a, f_b

    def cross_chunks(lo, hi):
        @pl.loop(lo, hi)
        def _(j):
            for l in BOTH:
                halves = their_chunk(l, j)
                for h in BOTH:
                    for a in BOTH:
                        cross_gu(l, j, h, a, halves[h]).start()

    @scope("ring_start")
    def ring_start(a):
        @on_stay
        def _():
            for u in PIECES:
                for dn in BOTH:
                    ring(a, dn, 0, u, t, own=True).start()
            for u in PIECES:
                for dn in BOTH:
                    d2d(a, dn, 7, u, t, own=True).start()

        @on_swap
        def _():
            for l in BOTH:
                cross(l, a).wait_recv()
            for i in BOTH:
                for u in PIECES:
                    for dn in BOTH:
                        ring(a, dn, i, u, send_blk(dn, i)).start()
            for l in BOTH:
                for u in PIECES:
                    for dn in BOTH:
                        d2d(a, dn, 6 + l, u, links[l]).start()

    def ring_step(a, k, pieces=PIECES):
        def body():
            for u in pieces:
                for dn in BOTH:
                    b = arr_blk(dn, k)
                    ring(a, dn, k, u, b).wait_recv()

                    def forward():
                        ring(a, dn, k + 1, u, b).start()

                    if 1 <= k <= 4:
                        forward()
                    elif k < 6:
                        on_stay(forward)
                    d2d(a, dn, k, u, b).start()

        with scope(f"ring_{a}_{k}"):
            if k == 6:
                on_stay(body)
            else:
                body()

    def ring_steps(start, end, i):
        def at(places, act):
            if any(start <= place < end for place in places):
                pl.when(start + i == places[0] * stay + places[1] * swap)(act)

        for k, places in enumerate(zip(*DY_AT)):
            at(places, functools.partial(ring_step, 0, 2 + k))
        at(X_START, lambda: ring_start(1))
        for k, places in enumerate(zip(*X_AT)):
            at(places, functools.partial(ring_step, 1, k // SUB, (k % SUB,)))
        at(SUMS_AT, lambda: rs_start(0))
        at(SUMS_AT, lambda: rs_short(0))

    def bounce(a, h, kb, out_):
        vm = dgu.at[pl.ds((2 * a + kb) * rb + h * hb, hb), :]
        cols = pl.ds(kb * kd, kd)
        if out_:
            return pltpu.make_async_copy(vm, gath[a].at[pl.ds(al(t * rb + h * hb, hb), hb), cols], lsem.at[0, h, 2 * a + kb])
        return pltpu.make_async_copy(ins[a].at[pl.ds(h * hb, hb), cols], vm, lsem.at[0, h, 2 * a + kb])

    def wd_load(src, kb):
        return pltpu.make_async_copy(src.at[:, pl.ds(kb * kd, kd)], wb.at[1, pl.ds(kb * ff, ff), :], wsem.at[kb])

    early = blocks // 2

    @on_swap
    def _():
        for j in (0, 2):
            for l in BOTH:
                cross(l, j).start()
        cross_chunks(0, early)

    @on_stay
    def _():
        for a in BOTH:
            for h in BOTH:
                for kb in BOTH:
                    bounce(a, h, kb, False).start()
        for kb in BOTH:
            wd_load(wd, kb).start()

    ring_start(0)

    @on_stay
    def _():
        for out_ in (False, True):
            for a in BOTH:
                for h in BOTH:
                    for kb in BOTH:
                        bounce(a, h, kb, out_).wait()
                        if not out_:
                            bounce(a, h, kb, True).start()

    ring_step(0, 0)

    @on_swap
    def _():
        cross_chunks(early, X_AFTER)
        for l in BOTH:
            cross(l, 1).start()
        cross_chunks(X_AFTER, blocks)

        @pl.loop(0, 4)
        def _(q):
            for a in BOTH:
                for l in BOTH:
                    cross_w(q, l, a).start()

    ring_step(0, 1)

    @on_swap
    def _():
        for l in BOTH:
            cross(l, 2).wait_recv()
        for kb in BOTH:
            wd_load(cwd, kb).start()

    def chunk_load(j, slot, h, what, f):
        rows = pl.ds(al(f * rb + h * hb, hb), hb)
        sem = lsem.at[slot, h, what]
        if what < 2:
            dst = wb.at[0, pl.ds(al(slot * 2 * rb + what * rb + h * hb, hb), hb), :]
            return pltpu.make_async_copy(dyg.at[rows, pl.ds(what * kd, kd)], dst, sem)
        dst = gu.at[slot, what % 2, pl.ds(h * hb, hb), :]
        src = ((gate, up), (cg, cu))[what // 4][what % 2]
        return pltpu.make_async_copy(src.at[rows, :], dst, lsem.at[slot, h, 2 + what % 2])

    @scope("chunk_start")
    def chunk_start(j):
        slot = parity(j)
        f_a, f_b, sw, k = chunk(j, team, r, t, cx, cy)
        halves = (f_a, f_b)

        @pl.when(sw != swap)
        def _():
            idx = jnp.where(j == 0, 7, jnp.where(j < 3, 5 + j, k))
            d2d_wait(0, idx)

        for h in BOTH:
            for kb in BOTH:
                chunk_load(j, slot, h, kb, halves[h]).start()

        @on_stay
        def _():
            for h in BOTH:
                for a in BOTH:
                    chunk_load(j, slot, h, 2 + a, halves[h]).start()

        @on_swap
        def _():
            pltpu.make_async_copy(dyg.at[pl.ds(0, hb)], xg.at[pl.ds(0, hb)], grecv.at[j]).wait()
            for h in BOTH:
                for a in BOTH:
                    chunk_load(j, slot, h, 4 + a, halves[h]).start()

    @scope("chunk")
    def chunk_compute(j):
        slot = parity(j)
        f_a, f_b, _, _ = chunk(j, team, r, t, cx, cy)
        halves = (f_a, f_b)
        for h in BOTH:
            for what in FOUR:
                chunk_load(j, slot, h, what, halves[h]).wait()
        for nt in BOTH:
            cols = pl.ds(nt * fh, fh)
            lhs = al(slot * 2 * rb, 2 * rb)
            dh = dot(wb[0, pl.ds(lhs, rb), :], wb[1, pl.ds(nt * fh, fh), :], NT)
            dh += dot(wb[0, pl.ds(lhs + rb, rb), :], wb[1, pl.ds(ff + nt * fh, fh), :], NT)
            g = gu[slot, 0, :, cols].astype(F32)
            u = gu[slot, 1, :, cols].astype(F32)
            sig = jax.nn.sigmoid(g)
            act = g * sig
            d_up = (dh * act).astype(BF16)
            d_gate = ((dh * u) * (sig * (1.0 + g * (1.0 - sig)))).astype(BF16)
            hidden = (act * u).astype(BF16)
            for h in BOTH:
                rows = pl.ds(al(halves[h] * rb + h * hb, hb), hb)
                part = slice(h * hb, (h + 1) * hb)
                dgu[rows, nt * fh : (nt + 1) * fh] = d_gate[part]
                dgu[rows, ff + nt * fh : ff + (nt + 1) * fh] = d_up[part]
                hid[rows, nt * fh : (nt + 1) * fh] = hidden[part]

    chunk_start(0)

    @on_stay
    def _():
        chunk_start(1)

    for kb in BOTH:
        wd_load(wd, kb).wait()

    @pl.loop(0, blocks)
    def _(j):
        chunk_compute(j)
        ring_steps(0, DOWN, j)

        @pl.when(j + 1 + stay < blocks)
        def _():
            chunk_start(j + 1 + stay)

    half = tok // 2

    def dy_cols(q, slot, th):
        return pltpu.make_async_copy(
            dyg.at[pl.ds(th * half, half), pl.ds(al(q * cq, cq), cq)],
            wb.at[slot, :, pl.ds(th * cq, cq)],
            wsem.at[2 * slot + th],
        )

    def down_at(q, ft):
        return pl.ds(al(ft * rb, rb), rb), pl.ds(al(q * cq, cq), cq)

    def down_buf(place):
        return gu.at[place // 2, parity(place)]

    def down_out(q, ft, to):
        return pltpu.make_async_copy(down_buf(ft), to.at[down_at(q, ft)], dsem.at[ft])

    def towards(l):
        return cx * (1 - l) + cy * l

    def down_remote(q, l):
        place = 2 * l + q % 2
        return remote(down_buf(place), od.at[down_at(q, 2 * l)], dsem.at[place], orecv.at[l], pdp, towards(l))

    def help_slot(q, l):
        return 2 * (q - 2) + l

    def help_remote(q, l):
        place = help_slot(q, l)
        return remote(out.at[place, 0], od.at[down_at(q, 2 * l + 1)], hsem.at[4 + place], orecv.at[l], dp, towards(l))

    def hidden_over(l):
        return remote(hid.at[:, pl.ds((2 * l + 1) * rb, rb)], hidr.at[:, pl.ds(l * rb, rb)], hsem.at[0], hsem.at[1], pdp, t)

    def hidden_in(sem):
        return pltpu.make_async_copy(hidr, hv, hsem.at[sem])

    def dy_start(q):
        for th in BOTH:
            dy_cols(q, q % 2, th).start()

    @scope("dw_down")
    def down_dot(q, lhs, ft):
        slot = q % 2
        cols = pl.ds(al(ft * rb, rb), rb)
        o = dot(lhs[0:half, cols], wb[slot, :, 0:cq], TN)
        o += dot(lhs[half:tok, cols], wb[slot, :, cq : 2 * cq], TN)
        return o.astype(BF16)

    def dy_wait(q):
        for th in BOTH:
            dy_cols(q, q % 2, th).wait()

    def w_load(q, a, src):
        rows = pl.ds(al(q * cq, cq), cq)
        slot = parity(q)
        return pltpu.make_async_copy(
            src.at[rows, :], wb.at[1, pl.ds(al(slot * cq, cq), cq), pl.ds(a * ff, ff)], wsem.at[4 + 2 * slot + a]
        )

    @scope("w_start")
    def w_start(q):
        @on_stay
        def _():
            for a in BOTH:
                w_load(q, a, (wg, wu)[a]).start()

        @on_swap
        def _():
            for a in BOTH:
                for l in BOTH:
                    cross_w(q, l, a).wait_recv()
                w_load(q, a, (cwg, cwu)[a]).start()

    @on_swap
    def _():
        for l in BOTH:
            hidden_over(l).start()

    dy_start(0)
    for q in BOTH:
        dy_wait(q)

        @pl.loop(0, 4)
        def _(i):
            ft = 2 * parity(i) + i // 2
            gu[ft // 2, parity(ft)] = down_dot(q, hid, ft)
            on_stay(lambda: down_out(q, ft, od).start())
            on_swap(lambda: down_out(q, ft, cwd).start())
            if q == 0:
                pl.when(i == 0)(lambda: dy_start(1))
            ring_steps(DOWN + 4 * q, DOWN + 4 * q + 4, i)

        for ft in FOUR:
            down_out(q, ft, od).wait()
        dy_start(2) if q == 0 else w_start(0)

        @on_swap
        def _():
            for l in BOTH:
                down_send(l, q).start()

    @on_stay
    def _():
        hidden_in(1).wait()
        hidden_in(2).start()

    def own_f(i):
        return blk_f(i, i)

    def other_f(i):
        return stay_f(i, team) * swap + swap_f(i, team) * stay

    def xf_out(step):
        q, i, o = step // ring_len, lax.rem(step, ring_len), parity(step)
        rows = pl.ds(al(own_f(i) * rb, rb), rb)
        return pltpu.make_async_copy(xf.at[o], dxp.at[rows, pl.ds(al(q * cq, cq), cq)], xfs.at[o])

    def xb_out(q, i, o):
        rows = pl.ds(al(other_f(i) * rb, rb), rb)
        return remote(out.at[o, 0], dxr.at[rows, pl.ds(al(q * cq, cq), cq)], xbs.at[o], drr.at[q // 2], pdp, t)

    def xb_send(step):
        return xb_out(step // ring_len, lax.rem(step, ring_len), parity(step))

    def rs_nbr(dn):
        return prv * (1 - dn) + nxt * dn

    def rs_send(dn, k, u, slot):
        return remote(rso.at[slot], rsl.at[dn, k, u], rss.at[slot], rsr.at[dn, k, u], dp, rs_nbr(dn))

    def slot_free(slot):
        pltpu.make_async_copy(rso.at[slot], rso.at[slot], rss.at[slot]).wait()

    def rs_part(which, slot, blk, dn, u):
        rows = pl.ds(al(blk * rb + dn * hb, hb), hb)
        cols = pl.ds(al(u * kd, kd), kd)
        src, dst = ((dxp, rpx), (dxr, rpr))[which]
        return pltpu.make_async_copy(src.at[rows, cols], dst.at[slot], rls.at[slot, which])

    def rs_sum(slot, to, received):
        @pl.loop(0, hb // 16)
        def _(i):
            rows = pl.ds(al(i * 16, 16), 16)
            v = rpx[slot, rows, :] + rpr[slot, rows, :].astype(F32)
            if received:
                v += rin[slot, rows, :].astype(F32)
            rso[to, rows, :] = v.astype(BF16)

    def rs_first(u, blks, k, base):
        for dn in BOTH:
            for which in BOTH:
                rs_part(which, dn, blks[dn], dn, u).start()
        for dn in BOTH:
            for which in BOTH:
                rs_part(which, dn, blks[dn], dn, u).wait()
            slot = base + 2 * u + dn
            rs_sum(dn, slot, False)
            rs_send(dn, k, u, slot).start()

    @scope("sum_start")
    def rs_start(u):
        all_of_it = pl.ds(0, ring_len * rb // 2)
        pltpu.make_async_copy(dyg.at[all_of_it], dxr.at[all_of_it], drr.at[u]).wait()
        rs_first(u, (blk_f(r + 1, r + 1), blk_f(r - 1, r + 5)), 0, 0)

    def rs_short(u):
        @on_swap
        @scope("sum_short")
        def _():
            rs_first(u, [swap_f(r - 1, team)] * 2, 5, 4)

    def rs_place(tt):
        m = tt // 4
        dn = parity(tt)
        pair = parity(tt // 2)
        early = jnp.where(m < 2, swap, 0)
        k = early * 5 * pair + (1 - early) * (m - swap)
        u = early * m + (1 - early) * pair
        to = 4 * (early * pair + (1 - early) * parity(m)) + 2 * u + dn
        late = jnp.where(k == 5, 1, 0)
        q_stay = (r - 6 + k) * (1 - dn) + (r + 6 - k) * dn
        q_swap = (r - 6 + k + late) * (1 - dn) + (r + 4 - k - late) * dn
        return m, k, u, dn, blk_f(q_stay, q_swap), to

    def rs_in(dn, k, u, slot):
        return pltpu.make_async_copy(rsl.at[dn, k, u], rin.at[slot], rls.at[slot, 2])

    @scope("sum_take")
    def rs_take(tt, slot):
        m, k, u, dn, blk, to = rs_place(tt)
        rs_part(0, slot, blk, dn, u).start()
        rs_part(1, slot, blk, dn, u).start()
        rs_send(dn, k, u, 0).wait_recv()
        rs_in(dn, k, u, slot).start()

    def last_sum(dn, u, slot):
        return pltpu.make_async_copy(rso.at[slot], (fin0, fin1)[dn].at[:, pl.ds(al(u * kd, kd), kd)], rss.at[slot])

    def rs_back(l, dn, u, slot):
        at = (pl.ds(al(dn * hb, hb), hb), pl.ds(al(u * kd, kd), kd))
        return remote(rso.at[slot], short.at[at], rss.at[slot], crr.at[dn, u], pdp, towards(l))

    @scope("sum_give")
    def rs_give(tt, slot):
        m, k, u, dn, blk, to = rs_place(tt)
        rs_part(0, slot, blk, dn, u).wait()
        rs_part(1, slot, blk, dn, u).wait()
        rs_in(dn, k, u, slot).wait()

        @pl.when((m != 1) | (swap == 1))
        def _():
            slot_free(to)

        rs_sum(slot, to, True)

        @pl.when(k < 4 + stay)
        def _():
            rs_send(dn, k + 1, u, to).start()

        for half_of in BOTH:

            @pl.when((k == 4 + stay) & (dn == half_of))
            def _():
                last_sum(half_of, u, to).start()

        @pl.when((swap == 1) & (k == 5))
        def _():
            rs_back(parity(1 - dn + odd), dn, u, to).start()

    def rest_put(dn, u):
        for which in BOTH:
            rs_part(which, 1, t, dn, u).start()
        for which in BOTH:
            rs_part(which, 1, t, dn, u).wait()

        @pl.loop(0, hb // 16)
        def _(i):
            rows = pl.ds(al(i * 16, 16), 16)
            rpx[1, rows, :] += rpr[1, rows, :].astype(F32)

        at = (pl.ds(al(dn * hb, hb), hb), pl.ds(al(u * kd, kd), kd))
        leave = pltpu.make_async_copy(rpx.at[1], rest.at[at], csem.at[1])
        leave.start()
        leave.wait()

    @pl.loop(0, 4 * ring_len)
    @scope("dx")
    def _(step):
        q = step // ring_len
        i = lax.rem(step, ring_len)
        o = parity(step)


        @pl.when(i == 0)
        def _():
            for a in BOTH:
                w_load(q, a, wg).wait()

        @pl.when((i == 7) & (q < 3))
        def _():
            w_start(q + 1)

        @pl.when(step >= 2)
        def _():
            xf_out(step - 2).wait()
            xb_send(step - 2).wait_send()

        w = pl.ds(al(parity(q) * cq, cq), cq)
        v = dot(jnp.concatenate([dgu[pl.ds(al(f(i) * rb, rb), rb), :] for f in (own_f, other_f)]), wb[1, w, :], NT)
        xf[o] = v[:rb]
        xf_out(step).start()
        out[o, 0] = v[rb:].astype(BF16)
        xb_send(step).start()
        ring_steps(TERMS, DONE, step)

    for step in (4 * ring_len - 2, 4 * ring_len - 1):
        xf_out(step).wait()
        xb_send(step).wait_send()

    dy_start(3)

    def down_put(q, ft, place):
        gu[place // 2, parity(place)] = down_dot(q, hid, ft)

    @on_stay
    def _():
        hidden_in(2).wait()
        for q in LATE:
            dy_wait(q)

            @pl.loop(0, 2)
            def _(i):
                out[help_slot(q, i), 0] = down_dot(q, hv, i)
                help_remote(q, i).start()
                if q == 2:
                    for ft in (i, 2 + i):
                        down_put(q, ft, ft)
                        down_out(q, ft, od).start()

            ring_step(1, 6, (q - 2,))

    rs_start(1)
    rs_short(1)
    pl.when(swap == 1)(lambda: dy_wait(2))
    for half_of in BOTH:
        q = 2 + half_of
        if half_of:

            @on_stay
            def _():
                for dn in BOTH:
                    rest_put(dn, 0)

            pl.when(swap == 1)(lambda: dy_wait(q))

        @pl.loop(0, 2)
        def _(i):
            tt = 2 * half_of + i
            rs_take(tt, 0)

            @on_stay
            def _():
                down_out(2, tt, od).wait()
                down_put(3, tt, tt)
                down_out(3, tt, od).start()

            @on_swap
            def _():
                down_put(q, 2 * i, 2 * i + half_of)
                down_remote(q, i).start()

            rs_give(tt, 0)

    for i in range(8):
        d2d_wait(1, i)

    def x_cols(i, th):
        slot = lax.rem(i, 4)
        return pltpu.make_async_copy(
            xg.at[pl.ds(th * half, half), pl.ds(al(i * rb, rb), rb)],
            wb.at[0, :, pl.ds(al(slot * 2 * rb + th * rb, rb), rb)],
            wsem.at[(4, 6)[th] + parity(slot) + 4 * (slot // 2)],
        )

    def x_start(i):
        for th in BOTH:
            x_cols(i, th).start()

    def dw_local(i, a):
        o = lax.rem(i, 4)
        return pltpu.make_async_copy(out.at[o, a], (og, ou)[a].at[pl.ds(al(i * rb, rb), rb), :], osem.at[o, a, 0])

    def dw_remote(i, a, l):
        o = lax.rem(i, 4)
        rows = pl.ds(al(i * rb, rb), rb)
        cols = pl.ds(l * fh, fh)
        return remote(out.at[o, a, :, cols], (og, ou)[a].at[rows, cols], osem.at[o, a, l], orecv.at[l], pdp, links[l])

    def dw_start(i, a):
        @on_stay
        def _():
            dw_local(i, a).start()

        @on_swap
        def _():
            for l in BOTH:
                dw_remote(i, a, l).start()

    @scope("dw_wait")
    def dw_wait(i, a):
        @on_stay
        def _():
            dw_local(i, a).wait()

        @on_swap
        def _():
            for l in BOTH:
                dw_remote(i, a, l).wait_send()

    for i in range(3):
        x_start(i)

    @on_stay
    def _():
        for q in LATE:
            for i in BOTH:
                help_remote(q, i).wait_send()

    @pl.loop(0, blocks)
    @scope("dw")
    def _(i):
        o = lax.rem(i, 4)

        @pl.when(i + 3 < blocks)
        def _():
            x_start(i + 3)

        for th in BOTH:
            x_cols(i, th).wait()
        rs_take(4 + i, 0)
        for a in BOTH:

            @pl.when(i >= 4)
            def _():
                dw_wait(i - 4, a)

            cols = slice(a * ff, (a + 1) * ff)
            v = dot(wb[0, :, pl.ds(al(o * 2 * rb, rb), rb)], dgu[0:half, cols], TN)
            v += dot(wb[0, :, pl.ds(al(o * 2 * rb + rb, rb), rb)], dgu[half:tok, cols], TN)
            out[o, a] = v.astype(BF16)
            dw_start(i, a)
            if a == 0:
                rs_give(4 + i, 0)

    @pl.loop(blocks + 4, 24)
    def _(tt):
        pl.when((stay == 1) & (tt < blocks + 6))(lambda: rest_put(parity(tt), 1))
        rs_take(tt, 0)
        rs_give(tt, 0)

    def sent(sem, rows):
        at = pl.ds(0, rows)
        pltpu.make_async_copy(dyg.at[at], xg.at[at], sem).wait()

    with scope("sent_dw"):
        for ft in FOUR:
            down_out(3, ft, od).wait()

        on_swap(lambda: hidden_in(0).wait())
        for i in range(blocks - 4, blocks):
            for a in BOTH:
                dw_wait(i, a)
    for a in BOTH:
        sent(dsend.at[a], ring_len * rb)
        on_stay(functools.partial(sent, rsend.at[a], 14 * hb))
        on_swap(functools.partial(sent, rsend.at[a], 12 * hb))

    @on_swap
    @scope("tail")
    def _():
        for l in BOTH:
            sent(csend.at[l], 13 * rb)
            sent(orecv.at[l], 6 * rb)
        for dn in BOTH:
            for u in BOTH:
                rs_back(0, dn, u, 0).wait_recv()

    with scope("slots"):
        for slot in range(8):
            slot_free(slot)


def last_hops(groups, n):
    ways = ([], [])
    for dp in range(groups):
        for t in range(n * n):
            x, y = divmod(t, n)
            team, odd = divmod((x + y) % n, 2)
            swap = (dp + team) % 2
            sg = odd if swap else 1 - odd
            step = 2 * sg - 1
            across, along = ((x + step) % n) * n + y, x * n + (y + step) % n
            to = (along, across) if odd else (across, along)
            if not swap:
                to = to[::-1]
            to_dp = dp + 1 - 2 * (dp % 2) if swap else dp
            for way, f in zip(ways, to):
                way.append((dp * n * n + t, to_dp * n * n + f))
    return ways


def copy_out(*refs):
    count = len(refs) // 4
    srcs, dsts, bufs, sems = (refs[i * count : (i + 1) * count] for i in FOUR)
    moves = []
    for src, dst, buf, sem in zip(srcs, dsts, bufs, sems):
        pieces = sem.shape[1]
        rows = src.shape[0] // pieces
        for i in range(pieces):
            at = pl.ds(i * rows, rows)
            moves.append(
                (
                    pltpu.make_async_copy(src.at[at], buf.at[at], sem.at[0, i]),
                    pltpu.make_async_copy(buf.at[at], dst.at[at], sem.at[1, i]),
                )
            )
    for load, _ in moves:
        load.start()
    for load, store in moves:
        load.wait()
        store.start()
    for _, store in moves:
        store.wait()


def solution(mesh):
    side = math.isqrt(mesh.shape["tp"])
    ways = last_hops(mesh.shape["dp"], side)

    def local(x, dy, gate, up, wg, wu, wd):
        rb, d = x.shape
        tok, ff = gate.shape
        hb, kd, blocks = rb // 2, d // 2, tok // rb

        def hbm(*shape, dtype=BF16):
            return jax.ShapeDtypeStruct(shape, dtype)

        outs = [
            hbm(hb, d), hbm(hb, d), hbm(rb, d, dtype=F32), hbm(rb, d),
            hbm(d, ff), hbm(d, ff), hbm(ff, d),
            hbm(tok, d), hbm(tok, d),
            hbm(tok, ff), hbm(tok, ff), hbm(d, ff), hbm(d, ff), hbm(ff, d),
            hbm(tok, d, dtype=F32), hbm(tok, d),
            hbm(2, 6, 2, hb, kd), hbm(tok, ff // 2),
        ]
        sem = pltpu.SemaphoreType.DMA
        scratch = [
            pltpu.VMEM((tok, 2 * ff), BF16),
            pltpu.VMEM((tok, ff), BF16),
            pltpu.VMEM((2, tok // 2, kd), BF16),
            pltpu.VMEM((2, 2, rb, ff), BF16),
            pltpu.VMEM((4, 2, rb, ff), BF16),
            pltpu.VMEM((2, rb, d // 4), F32),
            pltpu.VMEM((2, hb, kd), BF16),
            pltpu.VMEM((2, hb, kd), F32),
            pltpu.VMEM((2, hb, kd), BF16),
            pltpu.VMEM((8, hb, kd), BF16),
            pltpu.VMEM((tok, ff // 2), BF16),
            sem((2,)), sem((2, 2, 7, SUB)), sem((2,)), sem((2, 8)), sem((2,)), sem((2, 11)), sem((blocks,)),
            sem((12,)), sem((2, 2, 4)), sem((4, 2, 2)), sem((2,)),
            sem((2,)), sem((2,)), sem((2,)), sem((8,)), sem((2, 6, 2)), sem((2, 3)), sem((2, 2)), sem((2,)), sem((4,)), sem((8,)),
        ]
        res = pl.pallas_call(
            functools.partial(kernel, side),
            out_shape=outs,
            in_specs=[pl.BlockSpec(memory_space=pl.ANY)] * 7,
            out_specs=[pl.BlockSpec(memory_space=pl.ANY)] * len(outs),
            scratch_shapes=scratch,
            compiler_params=pltpu.CompilerParams(
                collective_id=0, has_side_effects=True, vmem_limit_bytes=64 * 2**20 - 2**16
            ),
            name="gated_mlp_backward",
        )(x, dy, gate, up, wg, wu, wd)
        fins, rest, short, res = res[:2], res[2], res[3], res[4:7]
        moved = [lax.ppermute(v, ("dp", "tp"), way) for v, way in zip(fins, ways)]
        anywhere = [pl.BlockSpec(memory_space=pl.ANY)] * len(res)
        grads = pl.pallas_call(
            copy_out,
            out_shape=[hbm(*v.shape) for v in res],
            in_specs=anywhere,
            out_specs=anywhere,
            scratch_shapes=[pltpu.VMEM(v.shape, BF16) for v in res]
            + [sem((2, max(1, v.size // (4 * rb * ff)))) for v in res],
            compiler_params=pltpu.CompilerParams(vmem_limit_bytes=48 * 2**20),
            cost_estimate=pl.CostEstimate(flops=10**10, bytes_accessed=6 * d * ff * 2, transcendentals=0),
            name="copy_out",
        )(*res)
        x, y = divmod(lax.axis_index("tp"), side)
        swap = (lax.axis_index("dp") + (x + y) % side // 2) % 2
        dx = (jnp.concatenate(moved).astype(F32) + jnp.where(swap == 1, short.astype(F32), rest)).astype(BF16)
        return dx, *grads

    rows, cols = P(("dp", "tp"), None), P("dp", "tp")
    return jax.shard_map(
        local,
        mesh=mesh,
        in_specs=(rows, rows, cols, cols, P(None, "tp"), P(None, "tp"), P("tp", None)),
        out_specs=(rows, cols, cols, rows),
        check_vma=False,
    )
```

```python
import functools
import math

import jax
import jax.numpy as jnp
from jax import lax
from jax.experimental import pallas as pl
from jax.experimental.pallas import tpu as pltpu
from jax.sharding import PartitionSpec as P

MESH = pl.DeviceIdType.MESH
BF16 = jnp.bfloat16
F32 = jnp.float32
NT = (((1,), (1,)), ((), ()))
TN = (((0,), (0,)), ((), ()))
BOTH = (0, 1)
LATE = (2, 3)
FOUR = range(4)
SUB = 2
PIECES = tuple(range(SUB))

X_AFTER = 9
NEVER = -1
DOWN, TERMS, DONE = 16, 24, 56
DY_AT = ((2, 4, 6, 8, 10), (2, 6, 8, 10, NEVER))
X_START = (10, 10)
X_AT = (
    (12, 12, 16, 17, 21, 25, 30, 34, 39, 43, 48, 53),
    (13, 15, 18, 21, 25, 30, 34, 38, 43, 48, 52, 55),
)
SUMS_AT = (55, 49)


scope = jax.named_scope


def parity(v):
    return lax.rem(v, 2)


def dot(a, b, dims):
    return lax.dot_general(a, b, dims, preferred_element_type=F32)


def kernel(
    side,
    x_in, dy_in, gate, up, wg, wu, wd,
    fin0, fin1, rest, short, og, ou, od, xg, dyg, cg, cu, cwg, cwu, cwd, dxp, dxr, rsl, hidr,
    dgu, hid, wb, gu, out, xf, rin, rpx, rpr, rso, hv,
    rsend, rrecv, dsend, drecv, csend, crecv, grecv,
    wsem, lsem, osem, orecv, xfs, xbs, drr, rss, rsr, rls, crr, csem, dsem, hsem,
):
    n = side
    ring_len = 2 * n
    rb, d_model = x_in.shape
    tok, ff = gate.shape
    hb = rb // 2
    fh = ff // 2
    kd = d_model // 2
    piece = hb // SUB
    blocks = tok // rb
    cq = d_model // 4

    t = lax.axis_index("tp")
    dp = lax.axis_index("dp")
    c = parity(dp)
    x = t // n
    y = lax.rem(t, n)
    s = lax.rem(x + y, n)
    team = s // 2
    odd = parity(s)
    swap = parity(c + team)
    stay = 1 - swap
    pdp = dp + 1 - 2 * c

    def on_stay(f):
        pl.when(stay == 1)(f)

    def on_swap(f):
        pl.when(swap == 1)(f)

    def wrap(v):
        return lax.rem(v + 2 * n, n)

    def wr(v):
        return lax.rem(v + 4 * ring_len, ring_len)

    def neighbours(x, y, odd):
        sg = 2 * odd - 1
        cx = wrap(x + sg) * n + y
        cy = x * n + wrap(y + sg)
        rx = wrap(x - sg) * n + y
        ry = x * n + wrap(y - sg)
        return cx, cy, rx * (1 - odd) + ry * odd, ry * (1 - odd) + rx * odd

    cx, cy, nxt, prv = neighbours(x, y, odd)
    links = (cx, cy)
    r = wr(2 * x - odd)

    def stay_f(q, team):
        q = wr(q)
        o = parity(q)
        bx = lax.rem((q + o) // 2, n)
        return bx * n + wrap(2 * team + o - bx)

    def swap_f(q, team):
        q = wr(q)
        o = parity(q)
        bx = lax.rem((q + 3 * o) // 2, n)
        return bx * n + wrap(2 * (1 - team) + (1 - o) - bx)

    def blk_f(q_stay, q_swap):
        return stay_f(q_stay, team) * stay + swap_f(q_swap, team) * swap

    def send_blk(dn, i):
        if dn == 0:
            return blk_f(r - i, r - i - (1 if i >= 1 else 0))
        return blk_f(r + i, r - 2 if i == 0 else r - 1 + i)

    def arr_blk(dn, k):
        if dn == 0:
            return blk_f(r - 1 - k, r - 1 if k == 0 else r - 2 - k)
        return blk_f(r + 1 + k, r - 1 if k == 0 else r + k)

    def chunk(j, team, r, t, cx, cy):
        k = jnp.maximum(j - 3, 0) // 2
        sw = jnp.where((j == 1) | (j == 2) | ((j >= 4) & (parity(j) == 0)), 1, 0)
        first = jnp.where(k == 0, 1, 0)
        st_a = jnp.where(j == 0, t, stay_f(r - 1 - k, team))
        st_b = jnp.where(j == 0, t, stay_f(r + 1 + k, team))
        entry = jnp.where(j == 1, cx, cy)
        sw_a = jnp.where(j < 3, entry, swap_f(r - 2 - k + first, team))
        sw_b = jnp.where(j < 3, entry, swap_f(r + k - first, team))
        return sw_a * sw + st_a * (1 - sw), sw_b * sw + st_b * (1 - sw), sw, k

    def al(v, m):
        return pl.multiple_of(v, m)

    bar = pltpu.get_barrier_semaphore()
    peers = ((dp, nxt), (dp, prv), (pdp, t), (pdp, cx), (pdp, cy), (dp, cx), (dp, cy))
    for p, f in peers:
        pl.semaphore_signal(bar, inc=1, device_id={"dp": p, "tp": f}, device_id_type=MESH)
    pl.semaphore_wait(bar, len(peers))

    ins = (dy_in, x_in)
    gath = (dyg, xg)
    nbr = (nxt, prv)

    def remote(src, dst, ssem, rsem, to_dp, to_tp):
        return pltpu.make_async_remote_copy(
            src, dst, ssem, rsem, device_id={"dp": to_dp, "tp": to_tp}, device_id_type=MESH
        )

    def rows_of(blk, dn, u):
        return pl.ds(al(blk * rb + (dn * hb + u * piece), piece), piece)

    def ring(a, dn, i, u, blk, own=False):
        dst = gath[a].at[rows_of(blk, dn, u)]
        src = ins[a].at[pl.ds(dn * hb + u * piece, piece)] if own else dst
        return remote(src, dst, rsend.at[a], rrecv.at[a, dn, i, u], dp, nbr[dn])

    def d2d(a, dn, i, u, blk, own=False):
        dst = gath[a].at[rows_of(blk, dn, u)]
        src = ins[a].at[pl.ds(dn * hb + u * piece, piece)] if own else dst
        return remote(src, dst, dsend.at[a], drecv.at[a, i], pdp, t)

    def d2d_wait(a, i):
        pltpu.make_async_copy(dyg.at[pl.ds(0, rb)], gath[a].at[pl.ds(0, rb)], drecv.at[a, i]).wait()

    def cross(l, j):
        cols = pl.ds(l * fh, fh)
        if j < 2:
            src, dst = ins[j], gath[j].at[pl.ds(al(t * rb, rb), rb)]
        else:
            src, dst = wd.at[cols], cwd.at[cols]
        return remote(src, dst, csend.at[l], crecv.at[l, j], pdp, links[l])

    def down_send(l, q):
        at = (pl.ds(l * fh, fh), pl.ds(q * cq, cq))
        return remote(cwd.at[at], od.at[at], csend.at[l], orecv.at[l], pdp, links[l])

    def cross_w(q, l, a):
        rows = pl.ds(al(q * cq, cq), cq)
        cols = pl.ds(l * fh, fh)
        src, dst = ((wg, cwg), (wu, cwu))[a]
        return remote(src.at[rows, cols], dst.at[rows, cols], csend.at[l], crecv.at[l, 3 + 2 * q + a], pdp, links[l])

    def cross_gu(l, j, h, a, f):
        rows = pl.ds(al(f * rb + h * hb, hb), hb)
        cols = pl.ds(l * fh, fh)
        src, dst = ((gate, cg), (up, cu))[a]
        return remote(src.at[rows, cols], dst.at[rows, cols], csend.at[l], grecv.at[j], pdp, links[l])

    def their_chunk(l, j):
        f = links[l]
        fx, fy = f // n, lax.rem(f, n)
        f_odd = 1 - odd
        f_cx, f_cy, _, _ = neighbours(fx, fy, f_odd)
        f_a, f_b, _, _ = chunk(j, 1 - team, wr(2 * fx - f_odd), f, f_cx, f_cy)
        return f_a, f_b

    def cross_chunks(lo, hi):
        @pl.loop(lo, hi)
        def _(j):
            for l in BOTH:
                halves = their_chunk(l, j)
                for h in BOTH:
                    for a in BOTH:
                        cross_gu(l, j, h, a, halves[h]).start()

    @scope("ring_start")
    def ring_start(a):
        @on_stay
        def _():
            for u in PIECES:
                for dn in BOTH:
                    ring(a, dn, 0, u, t, own=True).start()
            for u in PIECES:
                for dn in BOTH:
                    d2d(a, dn, 7, u, t, own=True).start()

        @on_swap
        def _():
            for l in BOTH:
                cross(l, a).wait_recv()
            for i in BOTH:
                for u in PIECES:
                    for dn in BOTH:
                        ring(a, dn, i, u, send_blk(dn, i)).start()
            for l in BOTH:
                for u in PIECES:
                    for dn in BOTH:
                        d2d(a, dn, 6 + l, u, links[l]).start()

    def ring_step(a, k, pieces=PIECES):
        def body():
            for u in pieces:
                for dn in BOTH:
                    b = arr_blk(dn, k)
                    ring(a, dn, k, u, b).wait_recv()

                    def forward():
                        ring(a, dn, k + 1, u, b).start()

                    if 1 <= k <= 4:
                        forward()
                    elif k < 6:
                        on_stay(forward)
                    d2d(a, dn, k, u, b).start()

        with scope(f"ring_{a}_{k}"):
            if k == 6:
                on_stay(body)
            else:
                body()

    def ring_steps(start, end, i):
        def at(places, act):
            if any(start <= place < end for place in places):
                pl.when(start + i == places[0] * stay + places[1] * swap)(act)

        for k, places in enumerate(zip(*DY_AT)):
            at(places, functools.partial(ring_step, 0, 2 + k))
        at(X_START, lambda: ring_start(1))
        for k, places in enumerate(zip(*X_AT)):
            at(places, functools.partial(ring_step, 1, k // SUB, (k % SUB,)))
        at(SUMS_AT, lambda: rs_start(0))
        at(SUMS_AT, lambda: rs_short(0))

    def bounce(a, h, kb, out_):
        vm = dgu.at[pl.ds((2 * a + kb) * rb + h * hb, hb), :]
        cols = pl.ds(kb * kd, kd)
        if out_:
            return pltpu.make_async_copy(vm, gath[a].at[pl.ds(al(t * rb + h * hb, hb), hb), cols], lsem.at[0, h, 2 * a + kb])
        return pltpu.make_async_copy(ins[a].at[pl.ds(h * hb, hb), cols], vm, lsem.at[0, h, 2 * a + kb])

    def wd_load(src, kb):
        return pltpu.make_async_copy(src.at[:, pl.ds(kb * kd, kd)], wb.at[1, pl.ds(kb * ff, ff), :], wsem.at[kb])

    early = blocks // 2

    @on_swap
    def _():
        for j in (0, 2):
            for l in BOTH:
                cross(l, j).start()
        cross_chunks(0, early)

    @on_stay
    def _():
        for a in BOTH:
            for h in BOTH:
                for kb in BOTH:
                    bounce(a, h, kb, False).start()
        for kb in BOTH:
            wd_load(wd, kb).start()

    ring_start(0)

    @on_stay
    def _():
        for out_ in (False, True):
            for a in BOTH:
                for h in BOTH:
                    for kb in BOTH:
                        bounce(a, h, kb, out_).wait()
                        if not out_:
                            bounce(a, h, kb, True).start()

    ring_step(0, 0)

    @on_swap
    def _():
        cross_chunks(early, X_AFTER)
        for l in BOTH:
            cross(l, 1).start()
        cross_chunks(X_AFTER, blocks)

        @pl.loop(0, 4)
        def _(q):
            for a in BOTH:
                for l in BOTH:
                    cross_w(q, l, a).start()

    ring_step(0, 1)

    @on_swap
    def _():
        for l in BOTH:
            cross(l, 2).wait_recv()
        for kb in BOTH:
            wd_load(cwd, kb).start()

    def chunk_load(j, slot, h, what, f):
        rows = pl.ds(al(f * rb + h * hb, hb), hb)
        sem = lsem.at[slot, h, what]
        if what < 2:
            dst = wb.at[0, pl.ds(al(slot * 2 * rb + what * rb + h * hb, hb), hb), :]
            return pltpu.make_async_copy(dyg.at[rows, pl.ds(what * kd, kd)], dst, sem)
        dst = gu.at[slot, what % 2, pl.ds(h * hb, hb), :]
        src = ((gate, up), (cg, cu))[what // 4][what % 2]
        return pltpu.make_async_copy(src.at[rows, :], dst, lsem.at[slot, h, 2 + what % 2])

    @scope("chunk_start")
    def chunk_start(j):
        slot = parity(j)
        f_a, f_b, sw, k = chunk(j, team, r, t, cx, cy)
        halves = (f_a, f_b)

        @pl.when(sw != swap)
        def _():
            idx = jnp.where(j == 0, 7, jnp.where(j < 3, 5 + j, k))
            d2d_wait(0, idx)

        for h in BOTH:
            for kb in BOTH:
                chunk_load(j, slot, h, kb, halves[h]).start()

        @on_stay
        def _():
            for h in BOTH:
                for a in BOTH:
                    chunk_load(j, slot, h, 2 + a, halves[h]).start()

        @on_swap
        def _():
            pltpu.make_async_copy(dyg.at[pl.ds(0, hb)], xg.at[pl.ds(0, hb)], grecv.at[j]).wait()
            for h in BOTH:
                for a in BOTH:
                    chunk_load(j, slot, h, 4 + a, halves[h]).start()

    @scope("chunk")
    def chunk_compute(j):
        slot = parity(j)
        f_a, f_b, _, _ = chunk(j, team, r, t, cx, cy)
        halves = (f_a, f_b)
        for h in BOTH:
            for what in FOUR:
                chunk_load(j, slot, h, what, halves[h]).wait()
        for nt in BOTH:
            cols = pl.ds(nt * fh, fh)
            lhs = al(slot * 2 * rb, 2 * rb)
            dh = dot(wb[0, pl.ds(lhs, rb), :], wb[1, pl.ds(nt * fh, fh), :], NT)
            dh += dot(wb[0, pl.ds(lhs + rb, rb), :], wb[1, pl.ds(ff + nt * fh, fh), :], NT)
            g = gu[slot, 0, :, cols].astype(F32)
            u = gu[slot, 1, :, cols].astype(F32)
            sig = jax.nn.sigmoid(g)
            act = g * sig
            d_up = (dh * act).astype(BF16)
            d_gate = ((dh * u) * (sig * (1.0 + g * (1.0 - sig)))).astype(BF16)
            hidden = (act * u).astype(BF16)
            for h in BOTH:
                rows = pl.ds(al(halves[h] * rb + h * hb, hb), hb)
                part = slice(h * hb, (h + 1) * hb)
                dgu[rows, nt * fh : (nt + 1) * fh] = d_gate[part]
                dgu[rows, ff + nt * fh : ff + (nt + 1) * fh] = d_up[part]
                hid[rows, nt * fh : (nt + 1) * fh] = hidden[part]

    chunk_start(0)

    @on_stay
    def _():
        chunk_start(1)

    for kb in BOTH:
        wd_load(wd, kb).wait()

    @pl.loop(0, blocks)
    def _(j):
        chunk_compute(j)
        ring_steps(0, DOWN, j)

        @pl.when(j + 1 + stay < blocks)
        def _():
            chunk_start(j + 1 + stay)

    half = tok // 2

    def dy_cols(q, slot, th):
        return pltpu.make_async_copy(
            dyg.at[pl.ds(th * half, half), pl.ds(al(q * cq, cq), cq)],
            wb.at[slot, :, pl.ds(th * cq, cq)],
            wsem.at[2 * slot + th],
        )

    def down_at(q, ft):
        return pl.ds(al(ft * rb, rb), rb), pl.ds(al(q * cq, cq), cq)

    def down_buf(place):
        return gu.at[place // 2, parity(place)]

    def down_out(q, ft, to):
        return pltpu.make_async_copy(down_buf(ft), to.at[down_at(q, ft)], dsem.at[ft])

    def towards(l):
        return cx * (1 - l) + cy * l

    def down_remote(q, l):
        place = 2 * l + q % 2
        return remote(down_buf(place), od.at[down_at(q, 2 * l)], dsem.at[place], orecv.at[l], pdp, towards(l))

    def help_slot(q, l):
        return 2 * (q - 2) + l

    def help_remote(q, l):
        place = help_slot(q, l)
        return remote(out.at[place, 0], od.at[down_at(q, 2 * l + 1)], hsem.at[4 + place], orecv.at[l], dp, towards(l))

    def hidden_over(l):
        return remote(hid.at[:, pl.ds((2 * l + 1) * rb, rb)], hidr.at[:, pl.ds(l * rb, rb)], hsem.at[0], hsem.at[1], pdp, t)

    def hidden_in(sem):
        return pltpu.make_async_copy(hidr, hv, hsem.at[sem])

    def dy_start(q):
        for th in BOTH:
            dy_cols(q, q % 2, th).start()

    @scope("dw_down")
    def down_dot(q, lhs, ft):
        slot = q % 2
        cols = pl.ds(al(ft * rb, rb), rb)
        o = dot(lhs[0:half, cols], wb[slot, :, 0:cq], TN)
        o += dot(lhs[half:tok, cols], wb[slot, :, cq : 2 * cq], TN)
        return o.astype(BF16)

    def dy_wait(q):
        for th in BOTH:
            dy_cols(q, q % 2, th).wait()

    def w_load(q, a, src):
        rows = pl.ds(al(q * cq, cq), cq)
        slot = parity(q)
        return pltpu.make_async_copy(
            src.at[rows, :], wb.at[1, pl.ds(al(slot * cq, cq), cq), pl.ds(a * ff, ff)], wsem.at[4 + 2 * slot + a]
        )

    @scope("w_start")
    def w_start(q):
        @on_stay
        def _():
            for a in BOTH:
                w_load(q, a, (wg, wu)[a]).start()

        @on_swap
        def _():
            for a in BOTH:
                for l in BOTH:
                    cross_w(q, l, a).wait_recv()
                w_load(q, a, (cwg, cwu)[a]).start()

    @on_swap
    def _():
        for l in BOTH:
            hidden_over(l).start()

    dy_start(0)
    for q in BOTH:
        dy_wait(q)

        @pl.loop(0, 4)
        def _(i):
            ft = 2 * parity(i) + i // 2
            gu[ft // 2, parity(ft)] = down_dot(q, hid, ft)
            on_stay(lambda: down_out(q, ft, od).start())
            on_swap(lambda: down_out(q, ft, cwd).start())
            if q == 0:
                pl.when(i == 0)(lambda: dy_start(1))
            ring_steps(DOWN + 4 * q, DOWN + 4 * q + 4, i)

        for ft in FOUR:
            down_out(q, ft, od).wait()
        dy_start(2) if q == 0 else w_start(0)

        @on_swap
        def _():
            for l in BOTH:
                down_send(l, q).start()

    @on_stay
    def _():
        hidden_in(1).wait()
        hidden_in(2).start()

    def own_f(i):
        return blk_f(i, i)

    def other_f(i):
        return stay_f(i, team) * swap + swap_f(i, team) * stay

    def xf_out(step):
        q, i, o = step // ring_len, lax.rem(step, ring_len), parity(step)
        rows = pl.ds(al(own_f(i) * rb, rb), rb)
        return pltpu.make_async_copy(xf.at[o], dxp.at[rows, pl.ds(al(q * cq, cq), cq)], xfs.at[o])

    def xb_out(q, i, o):
        rows = pl.ds(al(other_f(i) * rb, rb), rb)
        return remote(out.at[o, 0], dxr.at[rows, pl.ds(al(q * cq, cq), cq)], xbs.at[o], drr.at[q // 2], pdp, t)

    def xb_send(step):
        return xb_out(step // ring_len, lax.rem(step, ring_len), parity(step))

    def rs_nbr(dn):
        return prv * (1 - dn) + nxt * dn

    def rs_send(dn, k, u, slot):
        return remote(rso.at[slot], rsl.at[dn, k, u], rss.at[slot], rsr.at[dn, k, u], dp, rs_nbr(dn))

    def slot_free(slot):
        pltpu.make_async_copy(rso.at[slot], rso.at[slot], rss.at[slot]).wait()

    def rs_part(which, slot, blk, dn, u):
        rows = pl.ds(al(blk * rb + dn * hb, hb), hb)
        cols = pl.ds(al(u * kd, kd), kd)
        src, dst = ((dxp, rpx), (dxr, rpr))[which]
        return pltpu.make_async_copy(src.at[rows, cols], dst.at[slot], rls.at[slot, which])

    def rs_sum(slot, to, received):
        @pl.loop(0, hb // 16)
        def _(i):
            rows = pl.ds(al(i * 16, 16), 16)
            v = rpx[slot, rows, :] + rpr[slot, rows, :].astype(F32)
            if received:
                v += rin[slot, rows, :].astype(F32)
            rso[to, rows, :] = v.astype(BF16)

    def rs_first(u, blks, k, base):
        for dn in BOTH:
            for which in BOTH:
                rs_part(which, dn, blks[dn], dn, u).start()
        for dn in BOTH:
            for which in BOTH:
                rs_part(which, dn, blks[dn], dn, u).wait()
            slot = base + 2 * u + dn
            rs_sum(dn, slot, False)
            rs_send(dn, k, u, slot).start()

    @scope("sum_start")
    def rs_start(u):
        all_of_it = pl.ds(0, ring_len * rb // 2)
        pltpu.make_async_copy(dyg.at[all_of_it], dxr.at[all_of_it], drr.at[u]).wait()
        rs_first(u, (blk_f(r + 1, r + 1), blk_f(r - 1, r + 5)), 0, 0)

    def rs_short(u):
        @on_swap
        @scope("sum_short")
        def _():
            rs_first(u, [swap_f(r - 1, team)] * 2, 5, 4)

    def rs_place(tt):
        m = tt // 4
        dn = parity(tt)
        pair = parity(tt // 2)
        early = jnp.where(m < 2, swap, 0)
        k = early * 5 * pair + (1 - early) * (m - swap)
        u = early * m + (1 - early) * pair
        to = 4 * (early * pair + (1 - early) * parity(m)) + 2 * u + dn
        late = jnp.where(k == 5, 1, 0)
        q_stay = (r - 6 + k) * (1 - dn) + (r + 6 - k) * dn
        q_swap = (r - 6 + k + late) * (1 - dn) + (r + 4 - k - late) * dn
        return m, k, u, dn, blk_f(q_stay, q_swap), to

    def rs_in(dn, k, u, slot):
        return pltpu.make_async_copy(rsl.at[dn, k, u], rin.at[slot], rls.at[slot, 2])

    @scope("sum_take")
    def rs_take(tt, slot):
        m, k, u, dn, blk, to = rs_place(tt)
        rs_part(0, slot, blk, dn, u).start()
        rs_part(1, slot, blk, dn, u).start()
        rs_send(dn, k, u, 0).wait_recv()
        rs_in(dn, k, u, slot).start()

    def last_sum(dn, u, slot):
        return pltpu.make_async_copy(rso.at[slot], (fin0, fin1)[dn].at[:, pl.ds(al(u * kd, kd), kd)], rss.at[slot])

    def rs_back(l, dn, u, slot):
        at = (pl.ds(al(dn * hb, hb), hb), pl.ds(al(u * kd, kd), kd))
        return remote(rso.at[slot], short.at[at], rss.at[slot], crr.at[dn, u], pdp, towards(l))

    @scope("sum_give")
    def rs_give(tt, slot):
        m, k, u, dn, blk, to = rs_place(tt)
        rs_part(0, slot, blk, dn, u).wait()
        rs_part(1, slot, blk, dn, u).wait()
        rs_in(dn, k, u, slot).wait()

        @pl.when((m != 1) | (swap == 1))
        def _():
            slot_free(to)

        rs_sum(slot, to, True)

        @pl.when(k < 4 + stay)
        def _():
            rs_send(dn, k + 1, u, to).start()

        for half_of in BOTH:

            @pl.when((k == 4 + stay) & (dn == half_of))
            def _():
                last_sum(half_of, u, to).start()

        @pl.when((swap == 1) & (k == 5))
        def _():
            rs_back(parity(1 - dn + odd), dn, u, to).start()

    def rest_put(dn, u):
        for which in BOTH:
            rs_part(which, 1, t, dn, u).start()
        for which in BOTH:
            rs_part(which, 1, t, dn, u).wait()

        @pl.loop(0, hb // 16)
        def _(i):
            rows = pl.ds(al(i * 16, 16), 16)
            rpx[1, rows, :] += rpr[1, rows, :].astype(F32)

        at = (pl.ds(al(dn * hb, hb), hb), pl.ds(al(u * kd, kd), kd))
        leave = pltpu.make_async_copy(rpx.at[1], rest.at[at], csem.at[1])
        leave.start()
        leave.wait()

    @pl.loop(0, 4 * ring_len)
    @scope("dx")
    def _(step):
        q = step // ring_len
        i = lax.rem(step, ring_len)
        o = parity(step)


        @pl.when(i == 0)
        def _():
            for a in BOTH:
                w_load(q, a, wg).wait()

        @pl.when((i == 7) & (q < 3))
        def _():
            w_start(q + 1)

        @pl.when(step >= 2)
        def _():
            xf_out(step - 2).wait()
            xb_send(step - 2).wait_send()

        w = pl.ds(al(parity(q) * cq, cq), cq)
        v = dot(jnp.concatenate([dgu[pl.ds(al(f(i) * rb, rb), rb), :] for f in (own_f, other_f)]), wb[1, w, :], NT)
        xf[o] = v[:rb]
        xf_out(step).start()
        out[o, 0] = v[rb:].astype(BF16)
        xb_send(step).start()
        ring_steps(TERMS, DONE, step)

    for step in (4 * ring_len - 2, 4 * ring_len - 1):
        xf_out(step).wait()
        xb_send(step).wait_send()

    dy_start(3)

    def down_put(q, ft, place):
        gu[place // 2, parity(place)] = down_dot(q, hid, ft)

    @on_stay
    def _():
        hidden_in(2).wait()
        for q in LATE:
            dy_wait(q)

            @pl.loop(0, 2)
            def _(i):
                out[help_slot(q, i), 0] = down_dot(q, hv, i)
                help_remote(q, i).start()
                if q == 2:
                    for ft in (i, 2 + i):
                        down_put(q, ft, ft)
                        down_out(q, ft, od).start()

            ring_step(1, 6, (q - 2,))

    rs_start(1)
    rs_short(1)
    def x_cols(i, th):
        slot = lax.rem(i, 4)
        return pltpu.make_async_copy(
            xg.at[pl.ds(th * half, half), pl.ds(al(i * rb, rb), rb)],
            wb.at[0, :, pl.ds(al(slot * 2 * rb + th * rb, rb), rb)],
            wsem.at[(4, 6)[th] + parity(slot) + 4 * (slot // 2)],
        )

    def x_start(i):
        for th in BOTH:
            x_cols(i, th).start()

    pl.when(swap == 1)(lambda: dy_wait(2))
    for half_of in BOTH:
        q = 2 + half_of
        if half_of:

            @on_stay
            def _():
                for dn in BOTH:
                    rest_put(dn, 0)

            pl.when(swap == 1)(lambda: dy_wait(q))
            for i in range(8):
                d2d_wait(1, i)
            for i in range(3):
                x_start(i)

        @pl.loop(0, 2)
        def _(i):
            tt = 2 * half_of + i
            rs_take(tt, 0)

            @on_stay
            def _():
                down_out(2, tt, od).wait()
                down_put(3, tt, tt)
                down_out(3, tt, od).start()

            @on_swap
            def _():
                down_put(q, 2 * i, 2 * i + half_of)
                down_remote(q, i).start()

            rs_give(tt, 0)

    def dw_local(i, a):
        o = lax.rem(i, 4)
        return pltpu.make_async_copy(out.at[o, a], (og, ou)[a].at[pl.ds(al(i * rb, rb), rb), :], osem.at[o, a, 0])

    def dw_remote(i, a, l):
        o = lax.rem(i, 4)
        rows = pl.ds(al(i * rb, rb), rb)
        cols = pl.ds(l * fh, fh)
        return remote(out.at[o, a, :, cols], (og, ou)[a].at[rows, cols], osem.at[o, a, l], orecv.at[l], pdp, links[l])

    def dw_start(i, a):
        @on_stay
        def _():
            dw_local(i, a).start()

        @on_swap
        def _():
            for l in BOTH:
                dw_remote(i, a, l).start()

    @scope("dw_wait")
    def dw_wait(i, a):
        @on_stay
        def _():
            dw_local(i, a).wait()

        @on_swap
        def _():
            for l in BOTH:
                dw_remote(i, a, l).wait_send()

    @on_stay
    def _():
        for q in LATE:
            for i in BOTH:
                help_remote(q, i).wait_send()

    @pl.loop(0, blocks)
    @scope("dw")
    def _(i):
        o = lax.rem(i, 4)

        @pl.when(i + 3 < blocks)
        def _():
            x_start(i + 3)

        for th in BOTH:
            x_cols(i, th).wait()
        rs_take(4 + i, 0)
        for a in BOTH:

            @pl.when(i >= 4)
            def _():
                dw_wait(i - 4, a)

            cols = slice(a * ff, (a + 1) * ff)
            v = dot(wb[0, :, pl.ds(al(o * 2 * rb, rb), rb)], dgu[0:half, cols], TN)
            v += dot(wb[0, :, pl.ds(al(o * 2 * rb + rb, rb), rb)], dgu[half:tok, cols], TN)
            out[o, a] = v.astype(BF16)
            dw_start(i, a)
            if a == 0:
                rs_give(4 + i, 0)

    @pl.loop(blocks + 4, 24)
    def _(tt):
        pl.when((stay == 1) & (tt < blocks + 6))(lambda: rest_put(parity(tt), 1))
        rs_take(tt, 0)
        rs_give(tt, 0)

    def sent(sem, rows):
        at = pl.ds(0, rows)
        pltpu.make_async_copy(dyg.at[at], xg.at[at], sem).wait()

    with scope("sent_dw"):
        for ft in FOUR:
            down_out(3, ft, od).wait()

        on_swap(lambda: hidden_in(0).wait())
        for i in range(blocks - 4, blocks):
            for a in BOTH:
                dw_wait(i, a)
    for a in BOTH:
        sent(dsend.at[a], ring_len * rb)
        on_stay(functools.partial(sent, rsend.at[a], 14 * hb))
        on_swap(functools.partial(sent, rsend.at[a], 12 * hb))

    @on_swap
    @scope("tail")
    def _():
        for l in BOTH:
            sent(csend.at[l], 13 * rb)
            sent(orecv.at[l], 6 * rb)
        for dn in BOTH:
            for u in BOTH:
                rs_back(0, dn, u, 0).wait_recv()

    with scope("slots"):
        for slot in range(8):
            slot_free(slot)


def last_hops(groups, n):
    ways = ([], [])
    for dp in range(groups):
        for t in range(n * n):
            x, y = divmod(t, n)
            team, odd = divmod((x + y) % n, 2)
            swap = (dp + team) % 2
            sg = odd if swap else 1 - odd
            step = 2 * sg - 1
            across, along = ((x + step) % n) * n + y, x * n + (y + step) % n
            to = (along, across) if odd else (across, along)
            if not swap:
                to = to[::-1]
            to_dp = dp + 1 - 2 * (dp % 2) if swap else dp
            for way, f in zip(ways, to):
                way.append((dp * n * n + t, to_dp * n * n + f))
    return ways


def copy_out(*refs):
    count = len(refs) // 4
    srcs, dsts, bufs, sems = (refs[i * count : (i + 1) * count] for i in FOUR)
    moves = []
    for src, dst, buf, sem in zip(srcs, dsts, bufs, sems):
        pieces = sem.shape[1]
        rows = src.shape[0] // pieces
        for i in range(pieces):
            at = pl.ds(i * rows, rows)
            moves.append(
                (
                    pltpu.make_async_copy(src.at[at], buf.at[at], sem.at[0, i]),
                    pltpu.make_async_copy(buf.at[at], dst.at[at], sem.at[1, i]),
                )
            )
    for load, _ in moves:
        load.start()
    for load, store in moves:
        load.wait()
        store.start()
    for _, store in moves:
        store.wait()


def solution(mesh):
    side = math.isqrt(mesh.shape["tp"])
    ways = last_hops(mesh.shape["dp"], side)

    def local(x, dy, gate, up, wg, wu, wd):
        rb, d = x.shape
        tok, ff = gate.shape
        hb, kd, blocks = rb // 2, d // 2, tok // rb

        def hbm(*shape, dtype=BF16):
            return jax.ShapeDtypeStruct(shape, dtype)

        outs = [
            hbm(hb, d), hbm(hb, d), hbm(rb, d, dtype=F32), hbm(rb, d),
            hbm(d, ff), hbm(d, ff), hbm(ff, d),
            hbm(tok, d), hbm(tok, d),
            hbm(tok, ff), hbm(tok, ff), hbm(d, ff), hbm(d, ff), hbm(ff, d),
            hbm(tok, d, dtype=F32), hbm(tok, d),
            hbm(2, 6, 2, hb, kd), hbm(tok, ff // 2),
        ]
        sem = pltpu.SemaphoreType.DMA
        scratch = [
            pltpu.VMEM((tok, 2 * ff), BF16),
            pltpu.VMEM((tok, ff), BF16),
            pltpu.VMEM((2, tok // 2, kd), BF16),
            pltpu.VMEM((2, 2, rb, ff), BF16),
            pltpu.VMEM((4, 2, rb, ff), BF16),
            pltpu.VMEM((2, rb, d // 4), F32),
            pltpu.VMEM((2, hb, kd), BF16),
            pltpu.VMEM((2, hb, kd), F32),
            pltpu.VMEM((2, hb, kd), BF16),
            pltpu.VMEM((8, hb, kd), BF16),
            pltpu.VMEM((tok, ff // 2), BF16),
            sem((2,)), sem((2, 2, 7, SUB)), sem((2,)), sem((2, 8)), sem((2,)), sem((2, 11)), sem((blocks,)),
            sem((12,)), sem((2, 2, 4)), sem((4, 2, 2)), sem((2,)),
            sem((2,)), sem((2,)), sem((2,)), sem((8,)), sem((2, 6, 2)), sem((2, 3)), sem((2, 2)), sem((2,)), sem((4,)), sem((8,)),
        ]
        res = pl.pallas_call(
            functools.partial(kernel, side),
            out_shape=outs,
            in_specs=[pl.BlockSpec(memory_space=pl.ANY)] * 7,
            out_specs=[pl.BlockSpec(memory_space=pl.ANY)] * len(outs),
            scratch_shapes=scratch,
            compiler_params=pltpu.CompilerParams(
                collective_id=0, has_side_effects=True, vmem_limit_bytes=64 * 2**20 - 2**16
            ),
            name="gated_mlp_backward",
        )(x, dy, gate, up, wg, wu, wd)
        fins, rest, short, res = res[:2], res[2], res[3], res[4:7]
        moved = [lax.ppermute(v, ("dp", "tp"), way) for v, way in zip(fins, ways)]
        anywhere = [pl.BlockSpec(memory_space=pl.ANY)] * len(res)
        grads = pl.pallas_call(
            copy_out,
            out_shape=[hbm(*v.shape) for v in res],
            in_specs=anywhere,
            out_specs=anywhere,
            scratch_shapes=[pltpu.VMEM(v.shape, BF16) for v in res]
            + [sem((2, max(1, v.size // (4 * rb * ff)))) for v in res],
            compiler_params=pltpu.CompilerParams(vmem_limit_bytes=48 * 2**20),
            cost_estimate=pl.CostEstimate(flops=10**10, bytes_accessed=6 * d * ff * 2, transcendentals=0),
            name="copy_out",
        )(*res)
        x, y = divmod(lax.axis_index("tp"), side)
        swap = (lax.axis_index("dp") + (x + y) % side // 2) % 2
        dx = (jnp.concatenate(moved).astype(F32) + jnp.where(swap == 1, short.astype(F32), rest)).astype(BF16)
        return dx, *grads

    rows, cols = P(("dp", "tp"), None), P("dp", "tp")
    return jax.shard_map(
        local,
        mesh=mesh,
        in_specs=(rows, rows, cols, cols, P(None, "tp"), P(None, "tp"), P("tp", None)),
        out_specs=(rows, cols, cols, rows),
        check_vma=False,
    )
```
